128 devices in a mesh: dp: 1, fsdp: 128 (over z, y, x, core).
Axes of the slice: x: 4, y: 4, z: 4, core: 2. Of those that a mesh axis runs over, the one named last changes fastest.
Arguments:
- latents: bfloat16 [512, 256, 1152], P(('dp', 'fsdp'))
- cond_emb: bfloat16 [512, 1152], P(('dp', 'fsdp'))
- w_ada: bfloat16 [2, 1152, 6912], P(None, 'fsdp')
- b_ada: bfloat16 [2, 6912], replicated
- w_qkv: bfloat16 [2, 1152, 3456], P(None, 'fsdp')
- b_qkv: bfloat16 [2, 3456], replicated
- w_proj: bfloat16 [2, 1152, 1152], P(None, 'fsdp')
- b_proj: bfloat16 [2, 1152], replicated
- w_fc1: bfloat16 [2, 1152, 4608], P(None, 'fsdp')
- b_fc1: bfloat16 [2, 4608], replicated
- w_fc2: bfloat16 [2, 4608, 1152], P(None, 'fsdp')
- b_fc2: bfloat16 [2, 1152], replicated
Outputs:
- output: bfloat16 [512, 256, 1152], P(('dp', 'fsdp'))
All inputs are finite; a program needn't handle non-finite values.
Results may differ from the reference program's by a relative error of at most 0.0139485.
Values are sent between devices in bfloat16 or wider.
A program may use at most 1 GiB of HBM per device.

```python
import jax
import jax.numpy as jnp
from jax import lax

SAMPLES = 4
GROUP_SIZE = 128
HIDDEN = 1152
TOKENS = 256
HEADS = 16
LAYERS = 2
BATCH = GROUP_SIZE * SAMPLES
HEAD_DIM = HIDDEN // HEADS
MLP_DIM = 4 * HIDDEN
LN_EPS = 1e-6


def setup_inputs(seed: int = 0, part: int = 0) -> dict:
    base_key = jax.random.key(seed)
    part_key = jax.random.fold_in(base_key, part)
    key_lat, key_cond = jax.random.split(part_key, 2)
    weight_keys = jax.random.split(jax.random.key(seed + 1), 10)

    def draw_weight(key_weight, fan_in, fan_out):
        return (jax.random.normal(key_weight, (LAYERS, fan_in, fan_out), jnp.float32) * fan_in ** -0.5).astype(jnp.bfloat16)

    def draw_bias(key_bias, fan_out):
        return (0.3 * jax.random.normal(key_bias, (LAYERS, fan_out), jnp.float32)).astype(jnp.bfloat16)

    return {
        'latents': jax.random.normal(key_lat, (BATCH, TOKENS, HIDDEN), jnp.float32).astype(jnp.bfloat16),
        'cond_emb': jax.random.normal(key_cond, (BATCH, HIDDEN), jnp.float32).astype(jnp.bfloat16),
        'w_ada': draw_weight(weight_keys[0], HIDDEN, 6 * HIDDEN),
        'b_ada': draw_bias(weight_keys[1], 6 * HIDDEN),
        'w_qkv': draw_weight(weight_keys[2], HIDDEN, 3 * HIDDEN),
        'b_qkv': draw_bias(weight_keys[3], 3 * HIDDEN),
        'w_proj': draw_weight(weight_keys[4], HIDDEN, HIDDEN),
        'b_proj': draw_bias(weight_keys[5], HIDDEN),
        'w_fc1': draw_weight(weight_keys[6], HIDDEN, MLP_DIM),
        'b_fc1': draw_bias(weight_keys[7], MLP_DIM),
        'w_fc2': draw_weight(weight_keys[8], MLP_DIM, HIDDEN),
        'b_fc2': draw_bias(weight_keys[9], HIDDEN),
    }


def layer_norm(values_in):
    mean_val = jnp.mean(values_in, axis=-1, keepdims=True)
    centered = values_in - mean_val
    var_val = jnp.mean(centered * centered, axis=-1, keepdims=True)
    return centered * lax.rsqrt(var_val + LN_EPS)


def dit_block(tokens_in, cond_act, weights):
    w_ada, b_ada, w_qkv, b_qkv, w_proj, b_proj, w_fc1, b_fc1, w_fc2, b_fc2 = weights
    modulation = jnp.dot(cond_act[None, :], w_ada, preferred_element_type=jnp.float32)[0] + b_ada.astype(jnp.float32)
    modulation = modulation.astype(jnp.bfloat16).astype(jnp.float32)
    shift_a, scale_a, gate_a, shift_m, scale_m, gate_m = jnp.split(modulation, 6)
    resid_a = tokens_in.astype(jnp.float32)
    normed = (layer_norm(resid_a) * (1.0 + scale_a) + shift_a).astype(jnp.bfloat16)
    qkv_rows = (jnp.dot(normed, w_qkv, preferred_element_type=jnp.float32) + b_qkv.astype(jnp.float32)).astype(jnp.bfloat16)
    qkv_rows = qkv_rows.astype(jnp.float32).reshape(TOKENS, 3, HEADS, HEAD_DIM)
    scores = jnp.einsum('qhd,khd->hqk', qkv_rows[:, 0], qkv_rows[:, 1]) * (HEAD_DIM ** -0.5)
    attn_probs = jax.nn.softmax(scores, axis=-1).astype(jnp.bfloat16).astype(jnp.float32)
    attn_out = jnp.einsum('hqk,khd->qhd', attn_probs, qkv_rows[:, 2]).astype(jnp.bfloat16).reshape(TOKENS, HIDDEN)
    proj_out = jnp.dot(attn_out, w_proj, preferred_element_type=jnp.float32) + b_proj.astype(jnp.float32)
    resid_b = (resid_a + gate_a * proj_out).astype(jnp.bfloat16).astype(jnp.float32)
    normed_b = (layer_norm(resid_b) * (1.0 + scale_m) + shift_m).astype(jnp.bfloat16)
    pre_act = jnp.dot(normed_b, w_fc1, preferred_element_type=jnp.float32) + b_fc1.astype(jnp.float32)
    hidden_act = jax.nn.gelu(pre_act, approximate=True).astype(jnp.bfloat16)
    mlp_out = jnp.dot(hidden_act, w_fc2, preferred_element_type=jnp.float32) + b_fc2.astype(jnp.float32)
    return (resid_b + gate_m * mlp_out).astype(jnp.bfloat16)


def reference(latents, cond_emb, w_ada, b_ada, w_qkv, b_qkv, w_proj, b_proj, w_fc1, b_fc1, w_fc2, b_fc2):
    stacked = (w_ada, b_ada, w_qkv, b_qkv, w_proj, b_proj, w_fc1, b_fc1, w_fc2, b_fc2)

    def one_sample(sample_pair):
        tokens_in, cond_row = sample_pair
        cond_act = jax.nn.silu(cond_row.astype(jnp.float32)).astype(jnp.bfloat16)

        def layer_step(carry_tok, weights):
            return dit_block(carry_tok, cond_act, weights), None

        result, _ = lax.scan(layer_step, tokens_in, stacked)
        return result

    return lax.map(one_sample, (latents, cond_emb))
```

```python
import functools
import jax
import jax.numpy as jnp
from jax import lax
from jax.experimental import pallas as pl
from jax.experimental.pallas import tpu as pltpu
from jax.sharding import PartitionSpec

MESH = pl.DeviceIdType.MESH
NL = 2
LANE = 128
RING, GROUP = 4, 8
RUN, PLANE, HALF = 72, 288, 144
TILE, QT = 256, 512
F2_COLS = 5 * LANE
N_A = 4608
CUT_A = ((3, 2, 1), (2, 3, 1))
CUT_B = ((2, 3, 1),)
CUT_C = ((7, 7, 1),)
CUT_D = ((3, 2, 1),)
SUBS = {(l, k): cut for l, row in enumerate(((CUT_A, CUT_A, CUT_B), (CUT_A, CUT_C, CUT_D))) for k, cut in enumerate(row)}
STARTS = (3, 17, 31, 47, 71, 99, 3, 58)
COLOURS = (1, 2, 0)


def width(l, k):
    return LANE * sum(a + b + c for a, b, c in SUBS[l, k])


W_MOD = 7 * LANE
W_F2 = F2_COLS + LANE


class Pos:
    def __init__(self):
        me = lax.axis_index('fsdp')
        self.c = lax.rem(me, 2)
        self.x = lax.rem(me // 2, RING)
        self.y = lax.rem(me // GROUP, RING)
        self.z = me // 32

    def dev(self, z=None, y=None, x=None, c=None):
        z = self.z if z is None else z
        y = self.y if y is None else y
        x = self.x if x is None else x
        c = self.c if c is None else c
        return {'fsdp': ((z * RING + y) * RING + x) * 2 + c}


def step4(v, k):
    return lax.rem(v + (k + RING), RING)


class Comm:
    def __init__(self, ssem, rsem):
        self.ssem, self.rsem, self.n = ssem, rsem, 0

    def take(self, k):
        b = self.n
        self.n += k
        return b

    def copy(self, src, dst, i, dev):
        return pltpu.make_async_remote_copy(src_ref=src, dst_ref=dst, send_sem=self.ssem.at[i], recv_sem=self.rsem.at[i], device_id=dev, device_id_type=MESH)


class Ring:
    def __init__(self, comm, pos, axis, sel, half):
        self.comm, self.sel, self.half = comm, sel, half
        self.b = comm.take(RING)
        me = getattr(pos, axis)
        self.me, self.r, self.l, self.o = me, step4(me, 1), step4(me, -1), step4(me, 2)
        self.right, self.left = pos.dev(**{axis: self.r}), pos.dev(**{axis: self.l})

    def start(self):
        own = self.sel(self.me)
        self.comm.copy(own, own, self.b, self.right).start()
        self.comm.copy(own, own, self.b + 1, self.left).start()

    def mid(self):
        a = self.sel(self.l)
        self.comm.copy(a, a, self.b, self.right).wait_recv()
        h = self.half(self.l, 0)
        self.comm.copy(h, h, self.b + 2, self.right).start()
        a = self.sel(self.r)
        self.comm.copy(a, a, self.b + 1, self.left).wait_recv()
        h = self.half(self.r, 1)
        self.comm.copy(h, h, self.b + 3, self.left).start()

    def end(self):
        h = self.half(self.o, 0)
        self.comm.copy(h, h, self.b + 2, self.right).wait_recv()
        h = self.half(self.o, 1)
        self.comm.copy(h, h, self.b + 3, self.left).wait_recv()

    def drain(self):
        own = self.sel(self.me)
        self.comm.copy(own, own, self.b, self.right).wait_send()
        self.comm.copy(own, own, self.b + 1, self.left).wait_send()
        h = self.half(self.l, 0)
        self.comm.copy(h, h, self.b + 2, self.right).wait_send()
        h = self.half(self.r, 1)
        self.comm.copy(h, h, self.b + 3, self.left).wait_send()


def pack_unit(comm, pos, g, off, wa, wb, wc):
    base = pos.c * (N_A // 2) + off
    ca = pl.ds(pl.multiple_of(base, LANE), wa)
    cb = pl.ds(pl.multiple_of(base + wa, LANE), wb)

    def cc(i):
        return pl.ds(pl.multiple_of(base + wa + wb + i * wc, LANE), wc)

    x, y, z = pos.x, pos.y, pos.z
    two = (pl.ds(0, 2), pl.ds(2, 2))
    big = (pl.ds(0, HALF), pl.ds(HALF, HALF))
    rings_a = [Ring(comm, pos, 'y', lambda i: g.at[z, rows_of(i), ca], lambda i, h: g.at[z, rows_of(i, h), ca]),
               Ring(comm, pos, 'z', lambda i: g.at[i, :, ca], lambda i, h: g.at[i, big[h], ca])]
    rings_b = [Ring(comm, pos, 'z', lambda i: g.at[i, rows_of(y), cb], lambda i, h: g.at[i, rows_of(y, h), cb]),
               Ring(comm, pos, 'y', lambda i: g.at[:, rows_of(i), cb], lambda i, h: g.at[two[h], rows_of(i), cb])]
    rings_c = [Ring(comm, pos, 'y', lambda i: g.at[z, rows_of(i), cc(x)], lambda i, h: g.at[z, rows_of(i, h), cc(x)]),
               Ring(comm, pos, 'z', lambda i: g.at[i, :, cc(x)], lambda i, h: g.at[i, big[h], cc(x)]),
               Ring(comm, pos, 'x', lambda i: g.at[:, :, cc(i)], lambda i, h: g.at[two[h], :, cc(i)])]
    def across(c):
        b = c * (N_A // 2) + off
        return [g.at[:, :, pl.ds(pl.multiple_of(b + o, LANE), n)] for o, n in ((0, wa), (wa, wb), (wa + wb, RING * wc))]

    return (rings_a, rings_b, rings_c), across(pos.c), across(1 - pos.c)


def rows_of(y, h=None):
    o, n = {None: (0, RUN), 0: (0, 40), 1: (40, 32)}[h]
    return pl.ds(pl.multiple_of(y * RUN + o, GROUP), n)


def fc2_unit(comm, pos, g, wa):
    r0 = pos.c * HALF
    x, y, z = pos.x, pos.y, pos.z
    full = pl.ds(pl.multiple_of(r0, GROUP), HALF)
    rows = (pl.ds(pl.multiple_of(r0, GROUP), RUN), pl.ds(pl.multiple_of(r0 + RUN, GROUP), RUN))
    two = (pl.ds(0, 2), pl.ds(2, 2))
    ca, cb = pl.ds(0, wa), pl.ds(wa, F2_COLS - wa)

    def cc(i):
        return pl.ds(pl.multiple_of(F2_COLS + i * LANE, LANE), LANE)

    rings_a = [Ring(comm, pos, 'y', lambda i: g.at[z, i, full, ca], lambda i, h: g.at[z, i, rows[h], ca]),
               Ring(comm, pos, 'z', lambda i: g.at[i, :, full, ca], lambda i, h: g.at[i, two[h], full, ca])]
    rings_b = [Ring(comm, pos, 'z', lambda i: g.at[i, y, full, cb], lambda i, h: g.at[i, y, rows[h], cb]),
               Ring(comm, pos, 'y', lambda i: g.at[:, i, full, cb], lambda i, h: g.at[two[h], i, full, cb])]
    rings_c = [Ring(comm, pos, 'y', lambda i: g.at[z, i, full, cc(x)], lambda i, h: g.at[z, i, rows[h], cc(x)]),
               Ring(comm, pos, 'z', lambda i: g.at[i, :, full, cc(x)], lambda i, h: g.at[i, two[h], full, cc(x)]),
               Ring(comm, pos, 'x', lambda i: g.at[:, :, full, cc(i)], lambda i, h: g.at[two[h], :, full, cc(i)])]
    def across(c):
        r = pl.ds(pl.multiple_of(c * HALF, GROUP), HALF)
        return [g.at[:, :, r, k] for k in (ca, cb, pl.ds(F2_COLS, RING * LANE))]

    return (rings_a, rings_b, rings_c), across(pos.c), across(1 - pos.c)


class Unit:
    def __init__(self, comm, pos, parts):
        self.rings, self.mine, self.other = parts
        self.comm = comm
        self.k = comm.take(3)
        self.sib = pos.dev(c=1 - pos.c)

    def across(self, i, refs):
        return self.comm.copy(refs[i], refs[i], self.k + i, self.sib)

    def stage(self, i, n):
        r = self.rings[i]
        if n == 2 * len(r):
            r[-1].end()
            self.across(i, self.mine).start()
        elif n == 2 * len(r) + 1:
            self.across(i, self.other).wait_recv()
        elif n % 2:
            r[n // 2].mid()
        else:
            if n:
                r[n // 2 - 1].end()
            r[n // 2].start()

    def drain(self):
        for i in range(3):
            for r in self.rings[i]:
                r.drain()
            self.across(i, self.mine).wait_send()


def mod_rings(comm, pos, h):
    y, z = pos.y, pos.z
    two, big = (pl.ds(0, 2), pl.ds(2, 2)), (pl.ds(0, HALF), pl.ds(HALF, HALF))
    ca, cb = pl.ds(0, RING * LANE), pl.ds(RING * LANE, 3 * LANE)
    return ([Ring(comm, pos, 'z', lambda i: h.at[i, rows_of(y), ca], lambda i, k: h.at[i, rows_of(y, k), ca]),
             Ring(comm, pos, 'y', lambda i: h.at[:, rows_of(i), ca], lambda i, k: h.at[two[k], rows_of(i), ca])],
            [Ring(comm, pos, 'y', lambda i: h.at[z, rows_of(i), cb], lambda i, k: h.at[z, rows_of(i, k), cb]),
             Ring(comm, pos, 'z', lambda i: h.at[i, :, cb], lambda i, k: h.at[i, big[k], cb])])


def entry_barrier(pos):
    bar = pltpu.get_barrier_semaphore()
    peers = [pos.dev(x=step4(pos.x, k)) for k in (1, 2, 3)]
    peers += [pos.dev(x=step4(pos.x, k), c=1 - pos.c) for k in (0, 1, 2, 3)]
    peers += [pos.dev(y=step4(pos.y, k)) for k in (1, -1)]
    peers += [pos.dev(z=step4(pos.z, k)) for k in (1, -1)]
    for p in peers:
        pl.semaphore_signal(bar, inc=1, device_id=p, device_id_type=MESH)
    pl.semaphore_wait(bar, len(peers))


HIDDEN = 1152
ROWS = 1024
HEAD = 72
HEADS = 16
LN_EPS = 1e-6
LOG2E = 1.4426950408889634


def ln_mod(v, shift, scale):
    mean = jnp.mean(v, axis=-1, keepdims=True)
    cen = v - mean
    var = jnp.mean(cen * cen, axis=-1, keepdims=True)
    return ((cen * lax.rsqrt(var + LN_EPS)) * (1.0 + scale) + shift).astype(jnp.bfloat16)


def piece(m_ref, l, s, j):
    return m_ref[l, pl.ds(s, 1), j * HIDDEN:(j + 1) * HIDDEN]


LT = 128


def norm1(src, m_ref, l, u):
    def body(i, _):
        rows = pl.ds(pl.multiple_of(i * LT, LT), LT)
        s = i // (TILE // LT)
        u[rows, :] = ln_mod(src[rows, :].astype(jnp.float32), piece(m_ref, l, s, 0), piece(m_ref, l, s, 1))
        return 0
    lax.fori_loop(0, ROWS // LT, body, 0)


def qkv_tiles(u, w, b, l, big, tick):
    def tile(cols, width):
        wt = w[:, :, cols].reshape(HIDDEN, width)
        for r in range(0, ROWS, QT):
            acc = jnp.dot(u[r:r + QT, :], wt, preferred_element_type=jnp.float32)
            big[r:r + QT, cols] = (acc + b[l:l + 1, cols].astype(jnp.float32)).astype(jnp.bfloat16)

    def body(n, _):
        tile(pl.ds(pl.multiple_of(n * QT, QT), QT), QT)
        tick(n)
        return 0
    lax.fori_loop(0, 6, body, 0)
    tile(slice(6 * QT, 6 * QT + 384), 384)


def attend(big, o, tick, n=RING):
    lane = lax.broadcasted_iota(jnp.int32, (1, TILE), 1)
    cst = (HEAD ** -0.5) * LOG2E

    def body(s, _):
        rows = pl.ds(pl.multiple_of(s * TILE, TILE), TILE)
        cur, cur_t = None, -1
        for h in range(HEADS):
            st = HEAD * h
            t0 = st // LANE
            off = st - t0 * LANE
            wd = LANE if off + HEAD <= LANE else 2 * LANE
            lo = t0 * LANE
            keep = jnp.logical_and(lane[:, :wd] >= off, lane[:, :wd] < off + HEAD)
            msk = jnp.where(keep, 1.0, 0.0).astype(jnp.bfloat16)
            q = big[rows, lo:lo + wd] * msk
            k = big[rows, HIDDEN + lo:HIDDEN + lo + wd]
            v = big[rows, 2 * HIDDEN + lo:2 * HIDDEN + lo + wd]
            sc = lax.dot_general(q, k, (((1,), (1,)), ((), ())), preferred_element_type=jnp.float32)
            mx = jnp.max(sc, axis=-1, keepdims=True)
            e = jnp.exp2((sc - mx) * cst)
            inv = 1.0 / jnp.sum(e, axis=-1, keepdims=True)
            p = (e * inv).astype(jnp.bfloat16)
            r = jnp.dot(p, v, preferred_element_type=jnp.float32)
            first = r[:, :LANE]
            if cur_t == t0 and off > 0:
                first = jnp.where(lane[:, :LANE] >= off, first, cur)
            if wd == LANE:
                cur, cur_t = first, t0
                if off + HEAD == LANE:
                    o[rows, lo:lo + LANE] = cur.astype(jnp.bfloat16)
                    cur, cur_t = None, -1
            else:
                o[rows, lo:lo + LANE] = first.astype(jnp.bfloat16)
                cur, cur_t = r[:, LANE:], t0 + 1
        tick(s)
        return 0
    lax.fori_loop(0, n, body, 0)


def proj_tiles(o, w, b, m_ref, l, src, x1, u, tick):
    def body(s, _):
        rows = pl.ds(pl.multiple_of(s * TILE, TILE), TILE)
        y = jnp.dot(o[rows, :], w[:, :, 3 * HIDDEN:].reshape(HIDDEN, HIDDEN), preferred_element_type=jnp.float32) + b[l:l + 1, :].astype(jnp.float32)
        v = (src[rows, :].astype(jnp.float32) + piece(m_ref, l, s, 2) * y).astype(jnp.bfloat16)
        x1[rows, :] = v
        u[rows, :] = ln_mod(v.astype(jnp.float32), piece(m_ref, l, s, 3), piece(m_ref, l, s, RING))
        tick(s)
        return 0
    lax.fori_loop(0, RING, body, 0)


def gelu(v):
    return 0.5 * v * (1.0 + jnp.tanh(0.7978845608028654 * (v + 0.044715 * (v * v * v))))


def fc1_tiles(u, w, b, l, big, tick):
    def body(n, _):
        cols = pl.ds(pl.multiple_of(n * QT, QT), QT)
        wt = w[:, :, cols].reshape(HIDDEN, QT)
        for r in range(0, ROWS, QT):
            acc = jnp.dot(u[r:r + QT, :], wt, preferred_element_type=jnp.float32)
            big[r:r + QT, cols] = gelu(acc + b[l:l + 1, cols].astype(jnp.float32)).astype(jnp.bfloat16)
        tick(n)
        return 0
    lax.fori_loop(0, 9, body, 0)


def fc2_tiles(big, w, b, m_ref, l, x1, dst, tick):
    def body(s, _):
        rows = pl.ds(pl.multiple_of(s * TILE, TILE), TILE)
        y = jnp.dot(big[rows, :], w[...].reshape(RING * HIDDEN, HIDDEN), preferred_element_type=jnp.float32) + b[l:l + 1, :].astype(jnp.float32)
        dst[rows, :] = (x1[rows, :].astype(jnp.float32) + piece(m_ref, l, s, 5) * y).astype(jnp.bfloat16)
        tick(s)
        return 0
    lax.fori_loop(0, RING, body, 0)


class Fan:
    def __init__(self, comm, pos, src, dst):
        self.comm, self.pos, self.src, self.dst = comm, pos, src, dst
        self.b = comm.take(GROUP)
        self.p = pos.x * 2 + pos.c

    def peer(self, k):
        q = lax.rem(self.p + k + GROUP, GROUP)
        return q, self.pos.dev(x=q // 2, c=lax.rem(q, 2))

    def put(self, k):
        q, dev = self.peer(k)
        return self.comm.copy(self.src(q), self.dst.at[self.p], self.b + k, dev)

    def start(self):
        for k in ORDER:
            self.put(k).start()

    def wait(self):
        for k in ORDER:
            q, dev = self.peer(-k)
            self.comm.copy(self.src(q), self.dst.at[q], self.b + k, dev).wait_recv()

    def drain(self):
        for k in ORDER:
            self.put(k).wait_send()


ORDER = range(1, GROUP)


class Scatter:
    def __init__(self, comm, pos, pieces, dst):
        self.comm, self.pos, self.pieces, self.dst = comm, pos, pieces, dst
        self.n = len(pieces(0, 0, 0))
        self.b = comm.take(GROUP * self.n)

    def each(self):
        for c in range(2):
            for d in (1, 3, 2, 0):
                x = step4(self.pos.x, d)
                for i, (src, at) in enumerate(self.pieces(x, c, self.pos.c)):
                    yield c, d, i, x, src, at

    def ends(self, d, i, at):
        return self.dst.at[2 * self.pos.x + self.pos.c, :, at], self.comm.rsem.at[self.b + (self.pos.c * RING + d) * self.n + i]

    def far(self, c, d, i, x, src, at):
        dst, r = self.ends(d, i, at)
        return pltpu.make_async_remote_copy(src_ref=src, dst_ref=dst, send_sem=self.comm.ssem.at[self.b + (c * RING + d) * self.n + i], recv_sem=r,
                                            device_id=self.pos.dev(x=x, c=c), device_id_type=MESH)

    def near(self, c, d, i, x, src, at):
        return pltpu.make_async_copy(src, *self.ends(d, i, at))

    def start(self):
        for v in self.each():
            if v[1]:
                self.far(*v).start()
            else:
                pl.when(self.pos.c != v[0])(lambda v=v: self.far(*v).start())
                pl.when(self.pos.c == v[0])(lambda v=v: self.near(*v).start())

    def wait(self):
        for c, d, i, x, src, at in self.each():
            dst = self.dst.at[2 * step4(self.pos.x, -d) + c, :, at]
            pltpu.make_async_copy(src, dst, self.comm.rsem.at[self.b + (c * RING + d) * self.n + i]).wait()

    def drain(self):
        for v in self.each():
            if v[1]:
                self.far(*v).wait_send()
            else:
                pl.when(self.pos.c != v[0])(lambda v=v: self.far(*v).wait_send())


class Scatter2:
    def __init__(self, comm, pos, w, dst):
        self.comm, self.pos, self.w, self.dst = comm, pos, w, dst
        self.b = comm.take(GROUP)
        self.slot = lax.rem(pos.x, 2) * 2 + pos.c

    def each(self):
        for d in (1, 3, 2, 0):
            x = step4(self.pos.x, d)
            yield d, 0, x, self.w.at[:, pl.ds(0, F2_COLS)], pl.ds(0, F2_COLS)
            yield d, 1, x, self.w.at[:, pl.ds(pl.multiple_of((5 + x) * LANE, LANE), LANE)], pl.ds(F2_COLS, LANE)

    def ends(self, i, at):
        return self.dst.at[self.slot, :, at], self.comm.rsem.at[self.b + self.slot * 2 + i]

    def far(self, d, i, x, src, at):
        dst, r = self.ends(i, at)
        return pltpu.make_async_remote_copy(src_ref=src, dst_ref=dst, send_sem=self.comm.ssem.at[self.b + d * 2 + i], recv_sem=r,
                                            device_id=self.pos.dev(x=x, c=self.pos.x // 2), device_id_type=MESH)

    def near(self, d, i, x, src, at):
        return pltpu.make_async_copy(src, *self.ends(i, at))

    def start(self):
        mine = self.pos.c == self.pos.x // 2
        for v in self.each():
            if v[0]:
                self.far(*v).start()
            else:
                pl.when(jnp.logical_not(mine))(lambda v=v: self.far(*v).start())
                pl.when(mine)(lambda v=v: self.near(*v).start())

    def wait(self):
        for d, i, x, src, at in self.each():
            pltpu.make_async_copy(src, self.dst.at[d, :, at], self.comm.rsem.at[self.b + d * 2 + i]).wait()

    def drain(self):
        mine = self.pos.c == self.pos.x // 2
        for v in self.each():
            if v[0]:
                self.far(*v).wait_send()
            else:
                pl.when(jnp.logical_not(mine))(lambda v=v: self.far(*v).wait_send())


def pack_pieces(l, k, w_qkv, w_proj, w_fc1):
    def pieces(x, c, _):
        out, to = [], 0
        for o, n, step in slices(l, k):
            o += c * (N_A // 2)
            w = w_fc1 if k else w_qkv
            if k == 0 and o >= 3 * HIDDEN:
                w, o = w_proj, o - 3 * HIDDEN
            out.append((w.at[l, :, pl.ds(pl.multiple_of(o + x * step, LANE), n)], pl.ds(to, n)))
            to += n
        return out
    return pieces


def mod_pieces(l, w_ada):
    def pieces(x, c, _):
        return [(w_ada.at[l, :, pl.ds(pl.multiple_of(jnp.minimum(7 * (2 * x + c), 47) * LANE, LANE), W_MOD)], pl.ds(0, W_MOD))]
    return pieces


def rows72(recv, wide, packed, n):
    for p in range(GROUP):
        wide[9 * p:9 * p + 9, :n] = recv[p].astype(jnp.float32)
    packed[:, :n] = wide[:, :n].astype(jnp.bfloat16)


def slices(l, k):
    o, out = 0, []
    for a, b, c in SUBS[l, k]:
        out += [(o, (a + b) * LANE, 0), (o + (a + b) * LANE, c * LANE, c * LANE)]
        o += (a + b + RING * c) * LANE
    return out


def place_pack(pos, packed, g, l, k):
    base = pos.c * (N_A // 2)
    pairs, at = [], 0
    for o, n, step in slices(l, k):
        pairs.append((packed.at[:, pl.ds(at, n)], g.at[pos.z, rows_of(pos.y), pl.ds(pl.multiple_of(base + o + pos.x * step, LANE), n)]))
        at += n
    return pairs


class Modulation:
    def __init__(self, comm, pos, l, h, hv, s_all, b_ref, part, got, m, lsem):
        self.rings = mod_rings(comm, pos, h)
        self.l, self.hv, self.s_all, self.b, self.part, self.got, self.m = l, hv, s_all, b_ref, part, got, m
        self.load = pltpu.make_async_copy(h, hv, lsem)
        self.fan = Fan(comm, pos, lambda q: part.at[q], got)

    def ring(self, c, n):
        r = self.rings[c]
        if n % 2:
            r[n // 2].mid()
        else:
            if n:
                r[n // 2 - 1].end()
            if n < RING:
                r[n // 2].start()

    def drain(self):
        for c in self.rings:
            for q in c:
                q.drain()
        self.fan.drain()

    def stage(self, n):
        if n == 0:
            self.load.start()
        elif n == 1:
            self.load.wait()
            rows = self.s_all[...].reshape(64, HIDDEN).astype(jnp.bfloat16)
            w = self.hv[...].reshape(HIDDEN, W_MOD)
            v = jnp.dot(rows, w, preferred_element_type=jnp.float32) + self.b[self.l:self.l + 1, pl.ds(pl.multiple_of(jnp.minimum(7 * self.fan.p, 47) * LANE, LANE), W_MOD)].astype(jnp.float32)
            self.part[...] = v.astype(jnp.bfloat16).astype(jnp.float32).reshape(GROUP, GROUP, W_MOD)
            self.fan.start()
            self.got[self.fan.p] = self.part[self.fan.p]
        else:
            self.fan.wait()
            for q in range(7):
                self.m[self.l, :, W_MOD * q:W_MOD * (q + 1)] = self.got[q]
            self.m[self.l, :, 7 * W_MOD:6 * HIDDEN] = self.got[7][:, 2 * LANE:]


P, W, X, U, M, N, L, S = range(GROUP)
QKV, ATT, PROJ, FC1, FC2 = range(5)
STEPS = ((QKV, 6, 1.5, 0.8), (ATT, RING, 3.2, 0.0), (PROJ, RING, 1.3, 0.0), (FC1, 9, 1.8, 0.0), (FC2, RING, 3.9, 0.0))
LINK, ACROSS, HOP = 46.6e3, 600e3, 3.0
BLOCK = RUN * TILE


class Plan:
    def __init__(self):
        self.t, self.free, self.done, self.pend, self.slack = HOP, {}, set(), [], 0.0
        self.units = [(l, k, v) for l in range(NL) for k in range(3) for v in SUBS[l, k]]
        self.rank = [(3 * l + k, i) for i, (l, k, _) in enumerate(self.units)]
        self.landed, self.loaded, self.left = {}, {}, {}
        self.pre, self.slots = [], []
        for l in range(NL):
            for k in range(3):
                self.add(STARTS[3 * l + k], (P, l, k))
            self.add(STARTS[3 * NL + l], (P, l, 3))
        self.add(7.0, (S,))
        self.emit = self.pre
        for l in range(NL):
            self.until((N, l))
            self.t += 2.5
            for st, n, each, tail in STEPS:
                k = {QKV: 0, FC1: 1, FC2: 2}.get(st)
                if k is not None:
                    self.until((L, l, k))
                    self.t = max(self.t, self.loaded[l, k])
                for i in range(n):
                    self.t += each
                    if i == n - 1 and st >= PROJ:
                        self.done.add((L, l, st - PROJ, l))
                    self.emit = []
                    self.slack = 1.0
                    self.catch_up()
                    self.slots.append(((l, st, i), self.emit))
                self.t += tail

    def add(self, when, action):
        k = action[0]
        if k in (U, L):
            rank = self.rank[action[1]]
        elif k == S:
            rank = (0, -2)
        else:
            rank = (3 * action[1] + (action[2] if k in (P, W, X) and action[2] < 3 else 0), -1 if k == P and action[2] == 3 else 0)
        self.pend.append((when, rank, action))

    def due(self, p):
        return p[0] + (self.slack if p[2][0] in (U, M, W, X) else 0)

    def allowed(self, a):
        if a[0] == W and a[1]:
            return (X, a[1] - 1, a[2]) in self.done
        if a[0] == L and self.units[a[1]][0]:
            l, k, _ = self.units[a[1]]
            return (L, l - 1, k, l - 1) in self.done
        if a[0] == N and a[2] == 1:
            return (S,) in self.done
        if a[0] == N and a[2] == 0 and a[1]:
            return (N, a[1] - 1) in self.done
        return True

    def catch_up(self):
        while True:
            c = [p for p in self.pend if self.due(p) <= self.t and self.allowed(p[2])]
            if not c:
                return
            p = min(c, key=lambda v: (v[1], v[0]))
            self.pend.remove(p)
            self.emit.append(p[2])
            self.act(*p[2])

    def until(self, tag):
        self.slack = 0.0
        while True:
            self.catch_up()
            if tag in self.done:
                return
            self.t = max(self.t, min(p[0] for p in self.pend if self.allowed(p[2])))

    def both(self, link, size, rate=LINK):
        self.free[link] = max(self.t, self.free.get(link, self.t)) + size / rate
        return self.free[link] + HOP

    def ring(self, a, chain, size, n):
        if n == 2 * len(chain):
            return True
        big = size * RING ** (n // 2)
        self.add(self.both(chain[n // 2], big / 2 if n % 2 else big), a + (n + 1,))

    def act(self, kind, *n):
        if kind == P:
            l, k = n
            b = (W_F2, W_MOD)[k > 2] if k > 1 else width(l, k)
            self.add(self.both(0, 128 * b), (W, l, k))
        elif kind == W:
            self.t += 0.7
            self.add(self.t + 1.5, (X,) + n)
        elif kind == X:
            self.done.add((X,) + n)
            if n[1] == 3:
                for c in range(2):
                    self.add(self.t, (M, n[0], c, 0))
            for u, (l, k, _) in enumerate(self.units):
                if (l, k) == n:
                    for c in COLOURS:
                        self.add(self.t, (U, u, c, 0))
        elif kind == U:
            u, c, s = n
            l, k, v = self.units[u]
            size = v[c] * BLOCK * (2 if k == 2 else 1)
            chain = ((1, 2), (2, 1), (1, 2, 0))[c]
            if s == 2 * len(chain) + 1:
                self.landed[u] = self.landed.get(u, 0) + 1
                if self.landed[u] == 3:
                    self.add(self.t, (L, u))
            elif self.ring((U, u, c), chain, size, s):
                self.add(self.both(ACROSS, size * RING ** len(chain), ACROSS), (U, u, c, s + 1))
        elif kind == M:
            l, c, s = n
            if self.ring((M, l, c), ((2, 1), (1, 2))[c], (RING, 3)[c] * BLOCK, s):
                self.left[l] = self.left.get(l, 0) + 1
                if self.left[l] == 2:
                    self.add(self.t, (N, l, 0))
        elif kind == N:
            l, s = n
            if s == 2:
                self.done.add((N, l))
            else:
                self.t += 2.0 * s
                self.add(self.t + (4.5 if s else 2.5), (N, l, s + 1))
        elif kind == L:
            l, k, _ = self.units[n[0]]
            n_k = len(SUBS[l, k])
            self.loaded[l, k] = self.t + 1 + 3.5 / n_k
            self.left[L, l, k] = self.left.get((L, l, k), 0) + 1
            if self.left[L, l, k] == n_k:
                self.done.add((L, l, k))
        else:
            self.done.add((S,))


def step_kernel(x_ref, cond, w_ada, w_qkv, w_proj, w_fc1, w_fc2, ba, bq, bp, b1, b2, out, *refs):
    packs = (refs[0:RING], refs[RING:GROUP])
    u, x1, big, wq, wf, wg, rq0, rf0, rq1, rf1, rm, r2, wide, packed0, packed1, packed3, wide2, packed2, s_ref, s_all, hv, part, got, m, ssem, rsem, lsem, wsem = refs[GROUP:]
    plan = Plan()
    pos = Pos()
    comm = Comm(ssem, rsem)
    bufs = (wq, wf, wg)
    packed = (packed0, packed1, packed2, packed3)
    fan_s = Fan(comm, pos, lambda q: s_ref, s_all)
    fans, units, mods, loads, owner = [], [], [], [], []
    recvs = ((rq0, rf0, None, rm.at[0]), (rq1, rf1, None, rm.at[1]))
    for l in range(NL):
        gq, gf, g2, gm = packs[l]
        fans.append((Scatter(comm, pos, pack_pieces(l, 0, w_qkv, w_proj, w_fc1), recvs[l][0]), Scatter(comm, pos, pack_pieces(l, 1, w_qkv, w_proj, w_fc1), recvs[l][1]),
                     Scatter2(comm, pos, w_fc2.at[l], r2.at[l]), Scatter(comm, pos, mod_pieces(l, w_ada), recvs[l][3])))
        mods.append(Modulation(comm, pos, l, gm, hv, s_all, ba, part.at[l], got.at[l], m, lsem.at[10 + l]))
        for k in range(3):
            off, g, buf = 0, packs[l][k], bufs[k]
            for a, b, c in SUBS[l, k]:
                if k == 2:
                    units.append(Unit(comm, pos, fc2_unit(comm, pos, g, a * LANE)))
                    pairs = [(g, buf)]
                else:
                    units.append(Unit(comm, pos, pack_unit(comm, pos, g, off, a * LANE, b * LANE, c * LANE)))
                    n = (a + b + RING * c) * LANE
                    cols = [pl.ds(h * (N_A // 2) + off, n) for h in range(2)]
                    pairs = [(g.at[:, :, q], buf.at[:, :, q]) for q in cols]
                    off += n
                first = len(sum(loads, []))
                loads.append([pltpu.make_async_copy(s, d, wsem.at[first + i]) for i, (s, d) in enumerate(pairs)])
                owner.append((l, k))

    def ready(l, k):
        for own, cps in zip(owner, loads):
            if own == (l, k):
                for cp in cps:
                    cp.wait()

    def placing(l, i):
        g = packs[l][i]
        if i == 3:
            pairs = [(packed3.at[...], g.at[pos.z, rows_of(pos.y)])]
        elif i < 2:
            pairs = place_pack(pos, packed[i], g, l, i)
        else:
            full = pl.ds(pl.multiple_of(pos.c * HALF, GROUP), HALF)
            pairs = [(packed2.at[:, pl.ds(0, F2_COLS)], g.at[pos.z, pos.y, full, pl.ds(0, F2_COLS)]),
                     (packed2.at[:, pl.ds(F2_COLS, LANE)], g.at[pos.z, pos.y, full, pl.ds(pl.multiple_of((5 + pos.x) * LANE, LANE), LANE)])]
        return [pltpu.make_async_copy(a, b, lsem.at[(0, RING, 12, 14)[i] + k]) for k, (a, b) in enumerate(pairs)]

    def act(kind, *n):
        if kind == P:
            fans[n[0]][n[1]].start()
        elif kind == W:
            l, i = n
            fans[l][i].wait()
            if i == 2:
                for s in range(RING):
                    wide2[36 * s:36 * s + 36, :] = r2[l, s].astype(jnp.float32)
                packed2[...] = wide2[...].astype(jnp.bfloat16)
            else:
                rows72(recvs[l][i], wide, packed[i], W_MOD if i == 3 else width(l, i))
            for cp in placing(l, i):
                cp.start()
        elif kind == X:
            for cp in placing(*n):
                cp.wait()
        elif kind == U:
            units[n[0]].stage(n[1], n[2])
        elif kind == M:
            mods[n[0]].ring(n[1], n[2])
        elif kind == N:
            mods[n[0]].stage(n[1])
        elif kind == L:
            for cp in loads[n[0]]:
                cp.start()
        else:
            fan_s.wait()

    def ticker(l, stage):
        def tick(i):
            for (sl, ss, k), actions in plan.slots:
                if sl == l and ss == stage and actions:
                    @pl.when(i == k)
                    def _():
                        for v in actions:
                            act(*v)
        return tick

    s_ref[...] = jnp.zeros_like(s_ref)
    cv = cond[...].astype(jnp.float32)
    s_ref[0:RING, :] = jax.nn.silu(cv).astype(jnp.bfloat16).astype(jnp.float32)
    entry_barrier(pos)
    fan_s.start()
    s_all[fan_s.p] = s_ref[...]
    for v in plan.pre:
        act(*v)
    src = x_ref
    for l in range(NL):
        norm1(src, m, l, u)
        ready(l, 0)
        qkv_tiles(u, wq, bq, l, big, ticker(l, QKV))
        attend(big, u, ticker(l, ATT))
        proj_tiles(u, wq, bp, m, l, src, x1, u, ticker(l, PROJ))
        ready(l, 1)
        fc1_tiles(u, wf, b1, l, big, ticker(l, FC1))
        ready(l, 2)
        fc2_tiles(big, wg, b2, m, l, x1, out, ticker(l, FC2))
        src = out
    fan_s.drain()
    for l in range(NL):
        for f in fans[l]:
            f.drain()
        mods[l].drain()
    for v in units:
        v.drain()


N_SEM = GROUP + NL * (GROUP + GROUP + 16 + GROUP) + 16 * sum(len(v) for k, v in SUBS.items() if k[1] < 2) + 31 * sum(len(v) for v in SUBS.values())


def run_step(x, cond, w_ada, w_qkv, w_proj, w_fc1, w_fc2, ba, bq, bp, b1, b2):
    bf, f32 = jnp.bfloat16, jnp.float32
    shapes = [(RING, PLANE, N_A), (RING, PLANE, N_A), (RING, RING, PLANE, HIDDEN), (RING, PLANE, W_MOD)] * NL
    hbm = pl.BlockSpec(memory_space=pl.ANY)
    vm = pl.BlockSpec(memory_space=pltpu.VMEM)
    dma = pltpu.SemaphoreType.DMA
    return pl.pallas_call(
        step_kernel,
        out_shape=[jax.ShapeDtypeStruct((ROWS, HIDDEN), bf)] + [jax.ShapeDtypeStruct(s, bf) for s in shapes],
        in_specs=[vm, vm] + [hbm] * 5 + [vm] * 5, out_specs=[vm] + [hbm] * GROUP,
        scratch_shapes=[pltpu.VMEM((ROWS, HIDDEN), bf), pltpu.VMEM((ROWS, HIDDEN), bf), pltpu.VMEM((ROWS, N_A), bf),
                        pltpu.VMEM((RING, PLANE, N_A), bf), pltpu.VMEM((RING, PLANE, N_A), bf), pltpu.VMEM((RING, RING, PLANE, HIDDEN), bf),
                        *[pltpu.VMEM((GROUP, 9, width(l, k)), bf) for l in range(NL) for k in range(2)], pltpu.VMEM((NL, GROUP, 9, W_MOD), bf), pltpu.VMEM((NL, RING, 36, W_F2), bf),
                        pltpu.VMEM((RUN, 2048), f32), pltpu.VMEM((RUN, 2048), bf), pltpu.VMEM((RUN, 2048), bf), pltpu.VMEM((RUN, W_MOD), bf), pltpu.VMEM((HALF, W_F2), f32), pltpu.VMEM((HALF, W_F2), bf),
                        pltpu.VMEM((GROUP, HIDDEN), f32), pltpu.VMEM((GROUP, GROUP, HIDDEN), f32), pltpu.VMEM((RING, PLANE, W_MOD), bf), pltpu.VMEM((NL, GROUP, GROUP, W_MOD), f32), pltpu.VMEM((NL, GROUP, GROUP, W_MOD), f32),
                        pltpu.VMEM((NL, GROUP, 6 * HIDDEN), f32), dma((N_SEM,)), dma((N_SEM,)), dma((16,)), dma((2 * sum(len(v) for v in SUBS.values()),))],
        compiler_params=pltpu.CompilerParams(collective_id=0, has_side_effects=True, vmem_limit_bytes=67043328),
        name='dit_blocks',
    )(x, cond, w_ada, w_qkv, w_proj, w_fc1, w_fc2, ba, bq, bp, b1, b2)[0]


def solution(mesh):
    batch_spec = PartitionSpec(('dp', 'fsdp'), None, None)
    cond_spec = PartitionSpec(('dp', 'fsdp'), None)
    shard_spec = PartitionSpec(None, 'fsdp', None)
    bias_spec = PartitionSpec(None, None)

    def local_run(latents, cond_emb, w_ada, b_ada, w_qkv, b_qkv, w_proj, b_proj, w_fc1, b_fc1, w_fc2, b_fc2):
        y = run_step(latents.reshape(ROWS, HIDDEN), cond_emb, w_ada, w_qkv, w_proj, w_fc1, w_fc2, b_ada, b_qkv, b_proj, b_fc1, b_fc2)
        return y.reshape(latents.shape)

    in_specs = (batch_spec, cond_spec, shard_spec, bias_spec, shard_spec, bias_spec, shard_spec, bias_spec, shard_spec, bias_spec, shard_spec, bias_spec)
    return jax.shard_map(local_run, mesh=mesh, in_specs=in_specs, out_specs=batch_spec, check_vma=False)
```

```python
import functools
import jax
import jax.numpy as jnp
from jax import lax
from jax.experimental import pallas as pl
from jax.experimental.pallas import tpu as pltpu
from jax.sharding import PartitionSpec

MESH = pl.DeviceIdType.MESH
NL = 2
LANE = 128
RING, GROUP = 4, 8
RUN, PLANE, HALF = 72, 288, 144
TILE, QT = 256, 512
F2_COLS = 5 * LANE
N_A = 4608
CUT_A = ((3, 2, 1), (2, 3, 1))
CUT_B = ((2, 3, 1),)
CUT_D = ((3, 2, 1),)
SUBS = {(l, k): cut for l, row in enumerate(((CUT_A, CUT_A, CUT_B), (CUT_A, CUT_A, CUT_D))) for k, cut in enumerate(row)}
STARTS = (3, 16, 33, 9, 62, 86, 117, 78)
COLOURS = (1, 2, 0)


def width(l, k):
    return LANE * sum(a + b + c for a, b, c in SUBS[l, k])


W_MOD = 7 * LANE
W_F2 = F2_COLS + LANE


class Pos:
    def __init__(self):
        me = lax.axis_index('fsdp')
        self.c = lax.rem(me, 2)
        self.x = lax.rem(me // 2, RING)
        self.y = lax.rem(me // GROUP, RING)
        self.z = me // 32

    def dev(self, z=None, y=None, x=None, c=None):
        z = self.z if z is None else z
        y = self.y if y is None else y
        x = self.x if x is None else x
        c = self.c if c is None else c
        return {'fsdp': ((z * RING + y) * RING + x) * 2 + c}


def step4(v, k):
    return lax.rem(v + (k + RING), RING)


class Comm:
    def __init__(self, ssem, rsem):
        self.ssem, self.rsem, self.n = ssem, rsem, 0

    def take(self, k):
        b = self.n
        self.n += k
        return b

    def copy(self, src, dst, i, dev):
        return pltpu.make_async_remote_copy(src_ref=src, dst_ref=dst, send_sem=self.ssem.at[i], recv_sem=self.rsem.at[i], device_id=dev, device_id_type=MESH)


class Ring:
    def __init__(self, comm, pos, axis, sel, half):
        self.comm, self.sel, self.half = comm, sel, half
        self.b = comm.take(RING)
        me = getattr(pos, axis)
        self.me, self.r, self.l, self.o = me, step4(me, 1), step4(me, -1), step4(me, 2)
        self.right, self.left = pos.dev(**{axis: self.r}), pos.dev(**{axis: self.l})

    def start(self):
        own = self.sel(self.me)
        self.comm.copy(own, own, self.b, self.right).start()
        self.comm.copy(own, own, self.b + 1, self.left).start()

    def mid(self):
        a = self.sel(self.l)
        self.comm.copy(a, a, self.b, self.right).wait_recv()
        h = self.half(self.l, 0)
        self.comm.copy(h, h, self.b + 2, self.right).start()
        a = self.sel(self.r)
        self.comm.copy(a, a, self.b + 1, self.left).wait_recv()
        h = self.half(self.r, 1)
        self.comm.copy(h, h, self.b + 3, self.left).start()

    def end(self):
        h = self.half(self.o, 0)
        self.comm.copy(h, h, self.b + 2, self.right).wait_recv()
        h = self.half(self.o, 1)
        self.comm.copy(h, h, self.b + 3, self.left).wait_recv()

    def drain(self):
        own = self.sel(self.me)
        self.comm.copy(own, own, self.b, self.right).wait_send()
        self.comm.copy(own, own, self.b + 1, self.left).wait_send()
        h = self.half(self.l, 0)
        self.comm.copy(h, h, self.b + 2, self.right).wait_send()
        h = self.half(self.r, 1)
        self.comm.copy(h, h, self.b + 3, self.left).wait_send()


def pack_unit(comm, pos, g, off, wa, wb, wc):
    base = pos.c * (N_A // 2) + off
    ca = pl.ds(pl.multiple_of(base, LANE), wa)
    cb = pl.ds(pl.multiple_of(base + wa, LANE), wb)

    def cc(i):
        return pl.ds(pl.multiple_of(base + wa + wb + i * wc, LANE), wc)

    x, y, z = pos.x, pos.y, pos.z
    two = (pl.ds(0, 2), pl.ds(2, 2))
    big = (pl.ds(0, HALF), pl.ds(HALF, HALF))
    rings_a = [Ring(comm, pos, 'y', lambda i: g.at[z, rows_of(i), ca], lambda i, h: g.at[z, rows_of(i, h), ca]),
               Ring(comm, pos, 'z', lambda i: g.at[i, :, ca], lambda i, h: g.at[i, big[h], ca])]
    rings_b = [Ring(comm, pos, 'z', lambda i: g.at[i, rows_of(y), cb], lambda i, h: g.at[i, rows_of(y, h), cb]),
               Ring(comm, pos, 'y', lambda i: g.at[:, rows_of(i), cb], lambda i, h: g.at[two[h], rows_of(i), cb])]
    rings_c = [Ring(comm, pos, 'y', lambda i: g.at[z, rows_of(i), cc(x)], lambda i, h: g.at[z, rows_of(i, h), cc(x)]),
               Ring(comm, pos, 'z', lambda i: g.at[i, :, cc(x)], lambda i, h: g.at[i, big[h], cc(x)]),
               Ring(comm, pos, 'x', lambda i: g.at[:, :, cc(i)], lambda i, h: g.at[two[h], :, cc(i)])]
    def across(c):
        b = c * (N_A // 2) + off
        return [g.at[:, :, pl.ds(pl.multiple_of(b + o, LANE), n)] for o, n in ((0, wa), (wa, wb), (wa + wb, RING * wc))]

    return (rings_a, rings_b, rings_c), across(pos.c), across(1 - pos.c)


def rows_of(y, h=None):
    o, n = {None: (0, RUN), 0: (0, 40), 1: (40, 32)}[h]
    return pl.ds(pl.multiple_of(y * RUN + o, GROUP), n)


def fc2_unit(comm, pos, g, wa):
    r0 = pos.c * HALF
    x, y, z = pos.x, pos.y, pos.z
    full = pl.ds(pl.multiple_of(r0, GROUP), HALF)
    rows = (pl.ds(pl.multiple_of(r0, GROUP), RUN), pl.ds(pl.multiple_of(r0 + RUN, GROUP), RUN))
    two = (pl.ds(0, 2), pl.ds(2, 2))
    ca, cb = pl.ds(0, wa), pl.ds(wa, F2_COLS - wa)

    def cc(i):
        return pl.ds(pl.multiple_of(F2_COLS + i * LANE, LANE), LANE)

    rings_a = [Ring(comm, pos, 'y', lambda i: g.at[z, i, full, ca], lambda i, h: g.at[z, i, rows[h], ca]),
               Ring(comm, pos, 'z', lambda i: g.at[i, :, full, ca], lambda i, h: g.at[i, two[h], full, ca])]
    rings_b = [Ring(comm, pos, 'z', lambda i: g.at[i, y, full, cb], lambda i, h: g.at[i, y, rows[h], cb]),
               Ring(comm, pos, 'y', lambda i: g.at[:, i, full, cb], lambda i, h: g.at[two[h], i, full, cb])]
    rings_c = [Ring(comm, pos, 'y', lambda i: g.at[z, i, full, cc(x)], lambda i, h: g.at[z, i, rows[h], cc(x)]),
               Ring(comm, pos, 'z', lambda i: g.at[i, :, full, cc(x)], lambda i, h: g.at[i, two[h], full, cc(x)]),
               Ring(comm, pos, 'x', lambda i: g.at[:, :, full, cc(i)], lambda i, h: g.at[two[h], :, full, cc(i)])]
    def across(c):
        r = pl.ds(pl.multiple_of(c * HALF, GROUP), HALF)
        return [g.at[:, :, r, k] for k in (ca, cb, pl.ds(F2_COLS, RING * LANE))]

    return (rings_a, rings_b, rings_c), across(pos.c), across(1 - pos.c)


class Unit:
    def __init__(self, comm, pos, parts):
        self.rings, self.mine, self.other = parts
        self.comm = comm
        self.k = comm.take(3)
        self.sib = pos.dev(c=1 - pos.c)

    def across(self, i, refs):
        return self.comm.copy(refs[i], refs[i], self.k + i, self.sib)

    def stage(self, i, n):
        r = self.rings[i]
        if n == 2 * len(r):
            r[-1].end()
            self.across(i, self.mine).start()
        elif n == 2 * len(r) + 1:
            self.across(i, self.other).wait_recv()
        elif n % 2:
            r[n // 2].mid()
        else:
            if n:
                r[n // 2 - 1].end()
            r[n // 2].start()

    def drain(self):
        for i in range(3):
            for r in self.rings[i]:
                r.drain()
            self.across(i, self.mine).wait_send()


def mod_rings(comm, pos, h):
    y, z = pos.y, pos.z
    two, big = (pl.ds(0, 2), pl.ds(2, 2)), (pl.ds(0, HALF), pl.ds(HALF, HALF))
    ca, cb = pl.ds(0, RING * LANE), pl.ds(RING * LANE, 3 * LANE)
    return ([Ring(comm, pos, 'z', lambda i: h.at[i, rows_of(y), ca], lambda i, k: h.at[i, rows_of(y, k), ca]),
             Ring(comm, pos, 'y', lambda i: h.at[:, rows_of(i), ca], lambda i, k: h.at[two[k], rows_of(i), ca])],
            [Ring(comm, pos, 'y', lambda i: h.at[z, rows_of(i), cb], lambda i, k: h.at[z, rows_of(i, k), cb]),
             Ring(comm, pos, 'z', lambda i: h.at[i, :, cb], lambda i, k: h.at[i, big[k], cb])])


def entry_barrier(pos):
    bar = pltpu.get_barrier_semaphore()
    peers = [pos.dev(x=step4(pos.x, k)) for k in (1, 2, 3)]
    peers += [pos.dev(x=step4(pos.x, k), c=1 - pos.c) for k in (0, 1, 2, 3)]
    peers += [pos.dev(y=step4(pos.y, k)) for k in (1, -1)]
    peers += [pos.dev(z=step4(pos.z, k)) for k in (1, -1)]
    for p in peers:
        pl.semaphore_signal(bar, inc=1, device_id=p, device_id_type=MESH)
    pl.semaphore_wait(bar, len(peers))


HIDDEN = 1152
ROWS = 1024
HEAD = 72
HEADS = 16
LN_EPS = 1e-6
LOG2E = 1.4426950408889634


def ln_mod(v, shift, scale):
    mean = jnp.mean(v, axis=-1, keepdims=True)
    cen = v - mean
    var = jnp.mean(cen * cen, axis=-1, keepdims=True)
    return ((cen * lax.rsqrt(var + LN_EPS)) * (1.0 + scale) + shift).astype(jnp.bfloat16)


def piece(m_ref, l, s, j):
    return m_ref[l, pl.ds(s, 1), j * HIDDEN:(j + 1) * HIDDEN]


LT = 128


def norm1(src, m_ref, l, u):
    def body(i, _):
        rows = pl.ds(pl.multiple_of(i * LT, LT), LT)
        s = i // (TILE // LT)
        u[rows, :] = ln_mod(src[rows, :].astype(jnp.float32), piece(m_ref, l, s, 0), piece(m_ref, l, s, 1))
        return 0
    lax.fori_loop(0, ROWS // LT, body, 0)


def qkv_tiles(u, w, b, l, big, tick):
    def tile(cols, width):
        wt = w[:, :, cols].reshape(HIDDEN, width)
        for r in range(0, ROWS, QT):
            acc = jnp.dot(u[r:r + QT, :], wt, preferred_element_type=jnp.float32)
            big[r:r + QT, cols] = (acc + b[l:l + 1, cols].astype(jnp.float32)).astype(jnp.bfloat16)

    def body(n, _):
        tile(pl.ds(pl.multiple_of(n * QT, QT), QT), QT)
        tick(n)
        return 0
    lax.fori_loop(0, 6, body, 0)
    tile(slice(6 * QT, 6 * QT + 384), 384)


def attend(big, o, tick, n=RING):
    lane = lax.broadcasted_iota(jnp.int32, (1, TILE), 1)
    cst = (HEAD ** -0.5) * LOG2E

    def body(s, _):
        rows = pl.ds(pl.multiple_of(s * TILE, TILE), TILE)
        cur, cur_t = None, -1
        for h in range(HEADS):
            st = HEAD * h
            t0 = st // LANE
            off = st - t0 * LANE
            wd = LANE if off + HEAD <= LANE else 2 * LANE
            lo = t0 * LANE
            keep = jnp.logical_and(lane[:, :wd] >= off, lane[:, :wd] < off + HEAD)
            msk = jnp.where(keep, 1.0, 0.0).astype(jnp.bfloat16)
            q = big[rows, lo:lo + wd] * msk
            k = big[rows, HIDDEN + lo:HIDDEN + lo + wd]
            v = big[rows, 2 * HIDDEN + lo:2 * HIDDEN + lo + wd]
            sc = lax.dot_general(q, k, (((1,), (1,)), ((), ())), preferred_element_type=jnp.float32)
            mx = jnp.max(sc, axis=-1, keepdims=True)
            e = jnp.exp2((sc - mx) * cst)
            inv = 1.0 / jnp.sum(e, axis=-1, keepdims=True)
            p = (e * inv).astype(jnp.bfloat16)
            r = jnp.dot(p, v, preferred_element_type=jnp.float32)
            first = r[:, :LANE]
            if cur_t == t0 and off > 0:
                first = jnp.where(lane[:, :LANE] >= off, first, cur)
            if wd == LANE:
                cur, cur_t = first, t0
                if off + HEAD == LANE:
                    o[rows, lo:lo + LANE] = cur.astype(jnp.bfloat16)
                    cur, cur_t = None, -1
            else:
                o[rows, lo:lo + LANE] = first.astype(jnp.bfloat16)
                cur, cur_t = r[:, LANE:], t0 + 1
        tick(s)
        return 0
    lax.fori_loop(0, n, body, 0)


def proj_tiles(o, w, b, m_ref, l, src, x1, u, tick):
    def body(s, _):
        rows = pl.ds(pl.multiple_of(s * TILE, TILE), TILE)
        y = jnp.dot(o[rows, :], w[:, :, 3 * HIDDEN:].reshape(HIDDEN, HIDDEN), preferred_element_type=jnp.float32) + b[l:l + 1, :].astype(jnp.float32)
        v = (src[rows, :].astype(jnp.float32) + piece(m_ref, l, s, 2) * y).astype(jnp.bfloat16)
        x1[rows, :] = v
        u[rows, :] = ln_mod(v.astype(jnp.float32), piece(m_ref, l, s, 3), piece(m_ref, l, s, RING))
        tick(s)
        return 0
    lax.fori_loop(0, RING, body, 0)


def gelu(v):
    return 0.5 * v * (1.0 + jnp.tanh(0.7978845608028654 * (v + 0.044715 * (v * v * v))))


def fc1_tiles(u, w, b, l, big, tick):
    def body(n, _):
        cols = pl.ds(pl.multiple_of(n * QT, QT), QT)
        wt = w[:, :, cols].reshape(HIDDEN, QT)
        for r in range(0, ROWS, QT):
            acc = jnp.dot(u[r:r + QT, :], wt, preferred_element_type=jnp.float32)
            big[r:r + QT, cols] = gelu(acc + b[l:l + 1, cols].astype(jnp.float32)).astype(jnp.bfloat16)
        tick(n)
        return 0
    lax.fori_loop(0, 9, body, 0)


def fc2_tiles(big, w, b, m_ref, l, x1, dst, tick):
    def body(s, _):
        rows = pl.ds(pl.multiple_of(s * TILE, TILE), TILE)
        y = jnp.dot(big[rows, :], w[...].reshape(RING * HIDDEN, HIDDEN), preferred_element_type=jnp.float32) + b[l:l + 1, :].astype(jnp.float32)
        dst[rows, :] = (x1[rows, :].astype(jnp.float32) + piece(m_ref, l, s, 5) * y).astype(jnp.bfloat16)
        tick(s)
        return 0
    lax.fori_loop(0, RING, body, 0)


class Fan:
    def __init__(self, comm, pos, src, dst):
        self.comm, self.pos, self.src, self.dst = comm, pos, src, dst
        self.b = comm.take(GROUP)
        self.p = pos.x * 2 + pos.c

    def peer(self, k):
        q = lax.rem(self.p + k + GROUP, GROUP)
        return q, self.pos.dev(x=q // 2, c=lax.rem(q, 2))

    def put(self, k):
        q, dev = self.peer(k)
        return self.comm.copy(self.src(q), self.dst.at[self.p], self.b + k, dev)

    def start(self):
        for k in ORDER:
            self.put(k).start()

    def wait(self):
        for k in ORDER:
            q, dev = self.peer(-k)
            self.comm.copy(self.src(q), self.dst.at[q], self.b + k, dev).wait_recv()

    def drain(self):
        for k in ORDER:
            self.put(k).wait_send()


ORDER = range(1, GROUP)


class Scatter:
    def __init__(self, comm, pos, pieces, dst):
        self.comm, self.pos, self.pieces, self.dst = comm, pos, pieces, dst
        self.n = len(pieces(0, 0, 0))
        self.b = comm.take(GROUP * self.n)

    def each(self):
        for c in range(2):
            for d in (1, 3, 2, 0):
                x = step4(self.pos.x, d)
                for i, (src, at) in enumerate(self.pieces(x, c, self.pos.c)):
                    yield c, d, i, x, src, at

    def ends(self, d, i, at):
        return self.dst.at[2 * self.pos.x + self.pos.c, :, :, at], self.comm.rsem.at[self.b + (self.pos.c * RING + d) * self.n + i]

    def far(self, c, d, i, x, src, at):
        dst, r = self.ends(d, i, at)
        return pltpu.make_async_remote_copy(src_ref=src, dst_ref=dst, send_sem=self.comm.ssem.at[self.b + (c * RING + d) * self.n + i], recv_sem=r,
                                            device_id=self.pos.dev(x=x, c=c), device_id_type=MESH)

    def near(self, c, d, i, x, src, at):
        return pltpu.make_async_copy(src, *self.ends(d, i, at))

    def start(self):
        for v in self.each():
            if v[1]:
                self.far(*v).start()
            else:
                pl.when(self.pos.c != v[0])(lambda v=v: self.far(*v).start())
                pl.when(self.pos.c == v[0])(lambda v=v: self.near(*v).start())

    def wait(self):
        for c, d, i, x, src, at in self.each():
            dst = self.dst.at[2 * step4(self.pos.x, -d) + c, :, :, at]
            pltpu.make_async_copy(src, dst, self.comm.rsem.at[self.b + (c * RING + d) * self.n + i]).wait()

    def drain(self):
        for v in self.each():
            if v[1]:
                self.far(*v).wait_send()
            else:
                pl.when(self.pos.c != v[0])(lambda v=v: self.far(*v).wait_send())


class Scatter2:
    def __init__(self, comm, pos, w, dst):
        self.comm, self.pos, self.w, self.dst = comm, pos, w, dst
        self.b = comm.take(GROUP)
        self.slot = lax.rem(pos.x, 2) * 2 + pos.c

    def each(self):
        for d in (1, 3, 2, 0):
            x = step4(self.pos.x, d)
            yield d, 0, x, self.w.at[:, :, pl.ds(0, F2_COLS)], pl.ds(0, F2_COLS)
            yield d, 1, x, self.w.at[:, :, pl.ds(pl.multiple_of((5 + x) * LANE, LANE), LANE)], pl.ds(F2_COLS, LANE)

    def ends(self, i, at):
        return self.dst.at[self.slot, :, :, at], self.comm.rsem.at[self.b + self.slot * 2 + i]

    def far(self, d, i, x, src, at):
        dst, r = self.ends(i, at)
        return pltpu.make_async_remote_copy(src_ref=src, dst_ref=dst, send_sem=self.comm.ssem.at[self.b + d * 2 + i], recv_sem=r,
                                            device_id=self.pos.dev(x=x, c=self.pos.x // 2), device_id_type=MESH)

    def near(self, d, i, x, src, at):
        return pltpu.make_async_copy(src, *self.ends(i, at))

    def start(self):
        mine = self.pos.c == self.pos.x // 2
        for v in self.each():
            if v[0]:
                self.far(*v).start()
            else:
                pl.when(jnp.logical_not(mine))(lambda v=v: self.far(*v).start())
                pl.when(mine)(lambda v=v: self.near(*v).start())

    def wait(self):
        for d, i, x, src, at in self.each():
            pltpu.make_async_copy(src, self.dst.at[d, :, :, at], self.comm.rsem.at[self.b + d * 2 + i]).wait()

    def drain(self):
        mine = self.pos.c == self.pos.x // 2
        for v in self.each():
            if v[0]:
                self.far(*v).wait_send()
            else:
                pl.when(jnp.logical_not(mine))(lambda v=v: self.far(*v).wait_send())


def pack_pieces(k, w_qkv, w_proj, w_fc1):
    def pieces(x, c, _):
        out, to = [], 0
        for o, n, step in slices(0, k):
            o += c * (N_A // 2)
            w = w_fc1 if k else w_qkv
            if k == 0 and o >= 3 * HIDDEN:
                w, o = w_proj, o - 3 * HIDDEN
            out.append((w.at[:, :, pl.ds(pl.multiple_of(o + x * step, LANE), n)], pl.ds(to, n)))
            to += n
        return out
    return pieces


def mod_pieces(w_ada):
    def pieces(x, c, _):
        return [(w_ada.at[:, :, pl.ds(pl.multiple_of(jnp.minimum(7 * (2 * x + c), 47) * LANE, LANE), W_MOD)], pl.ds(0, W_MOD))]
    return pieces


def lay_rows(recv, l, wide, packed, n):
    devs, rows = recv.shape[0], recv.shape[1]

    def body(p, _):
        for r in range(rows):
            wide[pl.ds(p * rows + r, 1), :n] = recv[p, r].astype(jnp.float32)[l:l + 1, :]
        return 0
    lax.fori_loop(0, devs, body, 0)
    packed[:, :n] = wide[:, :n].astype(jnp.bfloat16)


def slices(l, k):
    o, out = 0, []
    for a, b, c in SUBS[l, k]:
        out += [(o, (a + b) * LANE, 0), (o + (a + b) * LANE, c * LANE, c * LANE)]
        o += (a + b + RING * c) * LANE
    return out


def place_pack(pos, packed, g, l, k):
    base = pos.c * (N_A // 2)
    pairs, at = [], 0
    for o, n, step in slices(l, k):
        pairs.append((packed.at[:, pl.ds(at, n)], g.at[pos.z, rows_of(pos.y), pl.ds(pl.multiple_of(base + o + pos.x * step, LANE), n)]))
        at += n
    return pairs


class Modulation:
    def __init__(self, comm, pos, l, h, hv, s_all, b_ref, part, got, m, lsem):
        self.rings = mod_rings(comm, pos, h)
        self.l, self.hv, self.s_all, self.b, self.part, self.got, self.m = l, hv, s_all, b_ref, part, got, m
        self.load = pltpu.make_async_copy(h, hv, lsem)
        self.fan = Fan(comm, pos, lambda q: part.at[q], got)

    def ring(self, c, n):
        r = self.rings[c]
        if n % 2:
            r[n // 2].mid()
        else:
            if n:
                r[n // 2 - 1].end()
            if n < RING:
                r[n // 2].start()

    def drain(self):
        for c in self.rings:
            for q in c:
                q.drain()
        self.fan.drain()

    def stage(self, n):
        if n == 0:
            self.load.start()
        elif n == 1:
            self.load.wait()
            rows = self.s_all[...].reshape(64, HIDDEN).astype(jnp.bfloat16)
            w = self.hv[...].reshape(HIDDEN, W_MOD)
            v = jnp.dot(rows, w, preferred_element_type=jnp.float32) + self.b[self.l:self.l + 1, pl.ds(pl.multiple_of(jnp.minimum(7 * self.fan.p, 47) * LANE, LANE), W_MOD)].astype(jnp.float32)
            self.part[...] = v.astype(jnp.bfloat16).astype(jnp.float32).reshape(GROUP, GROUP, W_MOD)
            self.fan.start()
            self.got[self.fan.p] = self.part[self.fan.p]
        else:
            self.fan.wait()
            for q in range(7):
                self.m[self.l, :, W_MOD * q:W_MOD * (q + 1)] = self.got[q]
            self.m[self.l, :, 7 * W_MOD:6 * HIDDEN] = self.got[7][:, 2 * LANE:]


P, W, X, U, M, N, L, S = range(GROUP)
QKV, ATT, PROJ, FC1, FC2 = range(5)
STEPS = ((QKV, 6, 1.5, 0.8), (ATT, RING, 3.2, 0.0), (PROJ, RING, 1.3, 0.0), (FC1, 9, 1.8, 0.0), (FC2, RING, 3.9, 0.0))
LINK, ACROSS, HOP = 46.6e3, 600e3, 3.0
BLOCK = RUN * TILE


class Plan:
    def __init__(self):
        self.t, self.free, self.done, self.pend, self.slack = HOP, {}, set(), [], 0.0
        self.units = [(l, k, v) for l in range(NL) for k in range(3) for v in SUBS[l, k]]
        self.rank = [(3 * l + k, i) for i, (l, k, _) in enumerate(self.units)]
        self.landed, self.loaded, self.left = {}, {}, {}
        self.pre, self.slots = [], []
        for k in range(RING):
            self.add(STARTS[k], (P, k))
        self.add(7.0, (S,))
        self.emit = self.pre
        for l in range(NL):
            self.until((N, l))
            self.t += 2.5
            for st, n, each, tail in STEPS:
                k = {QKV: 0, FC1: 1, FC2: 2}.get(st)
                if k is not None:
                    self.until((L, l, k))
                    self.t = max(self.t, self.loaded[l, k])
                for i in range(n):
                    self.t += each
                    if i == n - 1 and st >= PROJ:
                        self.done.add((L, l, st - PROJ, l))
                    self.emit = []
                    self.slack = 1.0
                    self.catch_up()
                    self.slots.append(((l, st, i), self.emit))
                self.t += tail

    def add(self, when, action):
        k = action[0]
        if k in (U, L):
            rank = self.rank[action[1]]
        elif k == S:
            rank = (0, -2)
        else:
            rank = (3 * action[1], 0) if k in (M, N) else (action[1] % 3, -action[1] // 3)
        self.pend.append((when, rank, action))

    def due(self, p):
        return p[0] + (self.slack if p[2][0] in (U, M, W, X) else 0)

    def allowed(self, a):
        if a[0] == L and self.units[a[1]][0]:
            l, k, _ = self.units[a[1]]
            return (L, l - 1, k, l - 1) in self.done
        if a[0] == N and a[2] == 1:
            return (S,) in self.done
        if a[0] == N and a[2] == 0 and a[1]:
            return (N, a[1] - 1) in self.done
        return True

    def catch_up(self):
        while True:
            c = [p for p in self.pend if self.due(p) <= self.t and self.allowed(p[2])]
            if not c:
                return
            p = min(c, key=lambda v: (v[1], v[0]))
            self.pend.remove(p)
            self.emit.append(p[2])
            self.act(*p[2])

    def until(self, tag):
        self.slack = 0.0
        while True:
            self.catch_up()
            if tag in self.done:
                return
            self.t = max(self.t, min(p[0] for p in self.pend if self.allowed(p[2])))

    def both(self, link, size, rate=LINK):
        self.free[link] = max(self.t, self.free.get(link, self.t)) + size / rate
        return self.free[link] + HOP

    def ring(self, a, chain, size, n):
        if n == 2 * len(chain):
            return True
        big = size * RING ** (n // 2)
        self.add(self.both(chain[n // 2], big / 2 if n % 2 else big), a + (n + 1,))

    def act(self, kind, *n):
        if kind == P:
            k, = n
            b = (W_F2, W_MOD)[k > 2] if k > 1 else width(0, k)
            self.add(self.both(0, HALF * b), (W, k))
        elif kind == W:
            self.t += 1.5
            self.add(self.t + 1.5, (X,) + n)
        elif kind == X:
            k, = n
            for l in range(NL):
                at = max(self.t, STARTS[RING + k] * l)
                if k == 3:
                    for c in range(2):
                        self.add(at, (M, l, c, 0))
                for u, own in enumerate(self.units):
                    if own[:2] == (l, k):
                        for c in COLOURS:
                            self.add(at, (U, u, c, 0))
        elif kind == U:
            u, c, s = n
            l, k, v = self.units[u]
            size = v[c] * BLOCK * (2 if k == 2 else 1)
            chain = ((1, 2), (2, 1), (1, 2, 0))[c]
            if s == 2 * len(chain) + 1:
                self.landed[u] = self.landed.get(u, 0) + 1
                if self.landed[u] == 3:
                    self.add(self.t, (L, u))
            elif self.ring((U, u, c), chain, size, s):
                self.add(self.both(ACROSS, size * RING ** len(chain), ACROSS), (U, u, c, s + 1))
        elif kind == M:
            l, c, s = n
            if self.ring((M, l, c), ((2, 1), (1, 2))[c], (RING, 3)[c] * BLOCK, s):
                self.left[l] = self.left.get(l, 0) + 1
                if self.left[l] == 2:
                    self.add(self.t, (N, l, 0))
        elif kind == N:
            l, s = n
            if s == 2:
                self.done.add((N, l))
            else:
                self.t += 2.0 * s
                self.add(self.t + (4.5 if s else 2.5), (N, l, s + 1))
        elif kind == L:
            l, k, _ = self.units[n[0]]
            n_k = len(SUBS[l, k])
            self.loaded[l, k] = self.t + 1 + 3.5 / n_k
            self.left[L, l, k] = self.left.get((L, l, k), 0) + 1
            if self.left[L, l, k] == n_k:
                self.done.add((L, l, k))
        else:
            self.done.add((S,))


def step_kernel(x_ref, cond, w_ada, w_qkv, w_proj, w_fc1, w_fc2, ba, bq, bp, b1, b2, out, *refs):
    packs = (refs[0:RING], refs[RING:GROUP])
    u, x1, big, wq, wf, wg, rq, rf, r2, rm, wide, wide2, s_ref, s_all, hv, part, got, m, ssem, rsem, lsem, wsem = refs[GROUP:-GROUP]
    packed = (refs[-GROUP:-RING], refs[-RING:])
    plan = Plan()
    pos = Pos()
    comm = Comm(ssem, rsem)
    bufs = (wq, wf, wg)
    fan_s = Fan(comm, pos, lambda q: s_ref, s_all)
    units, mods, loads, owner = [], [], [], []
    recvs = (rq, rf, r2, rm)
    fans = (Scatter(comm, pos, pack_pieces(0, w_qkv, w_proj, w_fc1), rq), Scatter(comm, pos, pack_pieces(1, w_qkv, w_proj, w_fc1), rf),
            Scatter2(comm, pos, w_fc2, r2), Scatter(comm, pos, mod_pieces(w_ada), rm))
    for l in range(NL):
        gq, gf, g2, gm = packs[l]
        mods.append(Modulation(comm, pos, l, gm, hv, s_all, ba, part.at[l], got.at[l], m, lsem.at[RING * GROUP + l]))
        for k in range(3):
            off, g, buf = 0, packs[l][k], bufs[k]
            for a, b, c in SUBS[l, k]:
                if k == 2:
                    units.append(Unit(comm, pos, fc2_unit(comm, pos, g, a * LANE)))
                    pairs = [(g, buf)]
                else:
                    units.append(Unit(comm, pos, pack_unit(comm, pos, g, off, a * LANE, b * LANE, c * LANE)))
                    n = (a + b + RING * c) * LANE
                    cols = [pl.ds(h * (N_A // 2) + off, n) for h in range(2)]
                    pairs = [(g.at[:, :, q], buf.at[:, :, q]) for q in cols]
                    off += n
                first = len(sum(loads, []))
                loads.append([pltpu.make_async_copy(s, d, wsem.at[first + i]) for i, (s, d) in enumerate(pairs)])
                owner.append((l, k))

    def ready(l, k):
        for own, cps in zip(owner, loads):
            if own == (l, k):
                for cp in cps:
                    cp.wait()

    def placing(i):
        pairs = []
        for l in range(NL):
            g, block = packs[l][i], packed[l][i]
            if i == 3:
                pairs.append((block, g.at[pos.z, rows_of(pos.y)]))
            elif i < 2:
                pairs += place_pack(pos, block, g, l, i)
            else:
                full = pl.ds(pl.multiple_of(pos.c * HALF, GROUP), HALF)
                pairs += [(block.at[:, pl.ds(0, F2_COLS)], g.at[pos.z, pos.y, full, pl.ds(0, F2_COLS)]),
                          (block.at[:, pl.ds(F2_COLS, LANE)], g.at[pos.z, pos.y, full, pl.ds(pl.multiple_of(F2_COLS + pos.x * LANE, LANE), LANE)])]
        return [pltpu.make_async_copy(a, b, lsem.at[i * GROUP + k]) for k, (a, b) in enumerate(pairs)]

    def act(kind, *n):
        if kind == P:
            fans[n[0]].start()
        elif kind == W:
            i, = n
            fans[i].wait()
            for l in range(NL):
                lay_rows(recvs[i], l, wide2 if i == 2 else wide, packed[l][i], recvs[i].shape[-1])
            for cp in placing(i):
                cp.start()
        elif kind == X:
            for cp in placing(*n):
                cp.wait()
        elif kind == U:
            units[n[0]].stage(n[1], n[2])
        elif kind == M:
            mods[n[0]].ring(n[1], n[2])
        elif kind == N:
            mods[n[0]].stage(n[1])
        elif kind == L:
            for cp in loads[n[0]]:
                cp.start()
        else:
            fan_s.wait()

    def ticker(l, stage):
        def tick(i):
            for (sl, ss, k), actions in plan.slots:
                if sl == l and ss == stage and actions:
                    @pl.when(i == k)
                    def _():
                        for v in actions:
                            act(*v)
        return tick

    s_ref[...] = jnp.zeros_like(s_ref)
    cv = cond[...].astype(jnp.float32)
    s_ref[0:RING, :] = jax.nn.silu(cv).astype(jnp.bfloat16).astype(jnp.float32)
    entry_barrier(pos)
    fan_s.start()
    s_all[fan_s.p] = s_ref[...]
    for v in plan.pre:
        act(*v)
    src = x_ref
    for l in range(NL):
        norm1(src, m, l, u)
        ready(l, 0)
        qkv_tiles(u, wq, bq, l, big, ticker(l, QKV))
        attend(big, u, ticker(l, ATT))
        proj_tiles(u, wq, bp, m, l, src, x1, u, ticker(l, PROJ))
        ready(l, 1)
        fc1_tiles(u, wf, b1, l, big, ticker(l, FC1))
        ready(l, 2)
        fc2_tiles(big, wg, b2, m, l, x1, out, ticker(l, FC2))
        src = out
    fan_s.drain()
    for v in fans:
        v.drain()
    for v in mods:
        v.drain()
    for v in units:
        v.drain()


N_SEM = GROUP * (3 + RING * NL) + 16 * sum(len(SUBS[0, k]) for k in range(2)) + 31 * sum(len(v) for v in SUBS.values()) + 8 * GROUP


def run_step(x, cond, w_ada, w_qkv, w_proj, w_fc1, w_fc2, ba, bq, bp, b1, b2):
    bf, f32 = jnp.bfloat16, jnp.float32
    shapes = [(RING, PLANE, N_A), (RING, PLANE, N_A), (RING, RING, PLANE, HIDDEN), (RING, PLANE, W_MOD)] * NL
    hbm = pl.BlockSpec(memory_space=pl.ANY)
    vm = pl.BlockSpec(memory_space=pltpu.VMEM)
    dma = pltpu.SemaphoreType.DMA
    wide = [width(0, k) for k in range(2)]
    return pl.pallas_call(
        step_kernel,
        out_shape=[jax.ShapeDtypeStruct((ROWS, HIDDEN), bf)] + [jax.ShapeDtypeStruct(s, bf) for s in shapes],
        in_specs=[vm, vm] + [hbm] * 5 + [vm] * 5, out_specs=[vm] + [hbm] * GROUP,
        scratch_shapes=[pltpu.VMEM((ROWS, HIDDEN), bf), pltpu.VMEM((ROWS, HIDDEN), bf), pltpu.VMEM((ROWS, N_A), bf),
                        pltpu.VMEM((RING, PLANE, N_A), bf), pltpu.VMEM((RING, PLANE, N_A), bf), pltpu.VMEM((RING, RING, PLANE, HIDDEN), bf),
                        pltpu.VMEM((GROUP, 9, NL, wide[0]), bf), pltpu.VMEM((GROUP, 9, NL, wide[1]), bf), pltpu.VMEM((RING, 36, NL, W_F2), bf), pltpu.VMEM((GROUP, 9, NL, W_MOD), bf),
                        pltpu.VMEM((RUN, max(wide)), f32), pltpu.VMEM((HALF, W_F2), f32),
                        pltpu.VMEM((GROUP, HIDDEN), f32), pltpu.VMEM((GROUP, GROUP, HIDDEN), f32), pltpu.VMEM((RING, PLANE, W_MOD), bf),
                        pltpu.VMEM((NL, GROUP, GROUP, W_MOD), f32), pltpu.VMEM((NL, GROUP, GROUP, W_MOD), f32), pltpu.VMEM((NL, GROUP, 6 * HIDDEN), f32),
                        dma((N_SEM,)), dma((N_SEM,)), dma((5 * GROUP,)), dma((2 * sum(len(v) for v in SUBS.values()),))]
        + [pltpu.VMEM((n, c), bf) for _ in range(NL) for n, c in ((RUN, wide[0]), (RUN, wide[1]), (HALF, W_F2), (RUN, W_MOD))],
        compiler_params=pltpu.CompilerParams(collective_id=0, has_side_effects=True, vmem_limit_bytes=67043328),
        name='dit_blocks',
    )(x, cond, w_ada, w_qkv, w_proj, w_fc1, w_fc2, ba, bq, bp, b1, b2)[0]


def solution(mesh):
    batch_spec = PartitionSpec(('dp', 'fsdp'), None, None)
    cond_spec = PartitionSpec(('dp', 'fsdp'), None)
    shard_spec = PartitionSpec(None, 'fsdp', None)
    bias_spec = PartitionSpec(None, None)

    def local_run(latents, cond_emb, w_ada, b_ada, w_qkv, b_qkv, w_proj, b_proj, w_fc1, b_fc1, w_fc2, b_fc2):
        y = run_step(latents.reshape(ROWS, HIDDEN), cond_emb, *[jnp.swapaxes(w, 0, 1) for w in (w_ada, w_qkv, w_proj, w_fc1, w_fc2)], b_ada, b_qkv, b_proj, b_fc1, b_fc2)
        return y.reshape(latents.shape)

    in_specs = (batch_spec, cond_spec, shard_spec, bias_spec, shard_spec, bias_spec, shard_spec, bias_spec, shard_spec, bias_spec, shard_spec, bias_spec)
    return jax.shard_map(local_run, mesh=mesh, in_specs=in_specs, out_specs=batch_spec, check_vma=False)
```

```python
import functools
import jax
import jax.numpy as jnp
from jax import lax
from jax.experimental import pallas as pl
from jax.experimental.pallas import tpu as pltpu
from jax.sharding import PartitionSpec

MESH = pl.DeviceIdType.MESH
NL = 2
LANE = 128
RING, GROUP = 4, 8
RUN, PLANE, HALF = 72, 288, 144
TILE, QT = 256, 512
F2_COLS = 5 * LANE
N_A = 4608
CUT_A = ((3, 2, 1), (2, 3, 1))
CUT_B = ((2, 3, 1),)
CUT_D = ((3, 2, 1),)
SUBS = {(l, k): cut for l, row in enumerate(((CUT_A, CUT_A, CUT_B), (CUT_A, CUT_A, CUT_D))) for k, cut in enumerate(row)}
STARTS = (3, 19, 35, 3, 64, 85, 117, 83)
COLOURS = (1, 2, 0)


def width(l, k):
    return LANE * sum(a + b + c for a, b, c in SUBS[l, k])


W_MOD = 7 * LANE
W_F2 = F2_COLS + LANE


class Pos:
    def __init__(self):
        me = lax.axis_index('fsdp')
        self.c = lax.rem(me, 2)
        self.x = lax.rem(me // 2, RING)
        self.y = lax.rem(me // GROUP, RING)
        self.z = me // 32

    def dev(self, z=None, y=None, x=None, c=None):
        z = self.z if z is None else z
        y = self.y if y is None else y
        x = self.x if x is None else x
        c = self.c if c is None else c
        return {'fsdp': ((z * RING + y) * RING + x) * 2 + c}


def step4(v, k):
    return lax.rem(v + (k + RING), RING)


class Comm:
    def __init__(self, ssem, rsem):
        self.ssem, self.rsem, self.n = ssem, rsem, 0

    def take(self, k):
        b = self.n
        self.n += k
        return b

    def copy(self, src, dst, i, dev):
        return pltpu.make_async_remote_copy(src_ref=src, dst_ref=dst, send_sem=self.ssem.at[i], recv_sem=self.rsem.at[i], device_id=dev, device_id_type=MESH)


class Ring:
    def __init__(self, comm, pos, axis, sel, half):
        self.comm, self.sel, self.half = comm, sel, half
        self.b = comm.take(6)
        me = getattr(pos, axis)
        self.me, self.r, self.l, self.o = me, step4(me, 1), step4(me, -1), step4(me, 2)
        self.right, self.left = pos.dev(**{axis: self.r}), pos.dev(**{axis: self.l})

    def hop(self, i, chip, h):
        ref = self.half(chip, h)
        return self.comm.copy(ref, ref, self.b + i, self.left if i % 2 else self.right)

    def sent(self):
        return [self.hop(i, self.me, h) for i, h in enumerate((0, 1, 1, 0))]

    def passed(self):
        return self.hop(RING, self.l, 0), self.hop(5, self.r, 1)

    def start(self):
        for m in self.sent():
            m.start()

    def mid(self):
        for i, m in enumerate(self.passed()):
            self.hop(i, (self.l, self.r)[i], i).wait_recv()
            m.start()

    def end(self):
        self.hop(2, self.l, 1).wait_recv()
        self.hop(3, self.r, 0).wait_recv()
        self.hop(RING, self.o, 0).wait_recv()
        self.hop(5, self.o, 1).wait_recv()

    def drain(self):
        for m in self.sent():
            m.wait_send()
        for m in self.passed():
            m.wait_send()


def pack_unit(comm, pos, g, off, wa, wb, wc):
    base = pos.c * (N_A // 2) + off
    ca = pl.ds(pl.multiple_of(base, LANE), wa)
    cb = pl.ds(pl.multiple_of(base + wa, LANE), wb)

    def cc(i):
        return pl.ds(pl.multiple_of(base + wa + wb + i * wc, LANE), wc)

    x, y, z = pos.x, pos.y, pos.z
    two = (pl.ds(0, 2), pl.ds(2, 2))
    big = (pl.ds(0, HALF), pl.ds(HALF, HALF))
    rings_a = [Ring(comm, pos, 'y', lambda i: g.at[z, rows_of(i), ca], lambda i, h: g.at[z, rows_of(i, h), ca]),
               Ring(comm, pos, 'z', lambda i: g.at[i, :, ca], lambda i, h: g.at[i, big[h], ca])]
    rings_b = [Ring(comm, pos, 'z', lambda i: g.at[i, rows_of(y), cb], lambda i, h: g.at[i, rows_of(y, h), cb]),
               Ring(comm, pos, 'y', lambda i: g.at[:, rows_of(i), cb], lambda i, h: g.at[two[h], rows_of(i), cb])]
    rings_c = [Ring(comm, pos, 'y', lambda i: g.at[z, rows_of(i), cc(x)], lambda i, h: g.at[z, rows_of(i, h), cc(x)]),
               Ring(comm, pos, 'z', lambda i: g.at[i, :, cc(x)], lambda i, h: g.at[i, big[h], cc(x)]),
               Ring(comm, pos, 'x', lambda i: g.at[:, :, cc(i)], lambda i, h: g.at[two[h], :, cc(i)])]
    def across(c):
        b = c * (N_A // 2) + off
        return [g.at[:, :, pl.ds(pl.multiple_of(b + o, LANE), n)] for o, n in ((0, wa), (wa, wb), (wa + wb, RING * wc))]

    return (rings_a, rings_b, rings_c), across(pos.c), across(1 - pos.c)


def rows_of(y, h=None):
    o, n = {None: (0, RUN), 0: (0, 40), 1: (40, 32)}[h]
    return pl.ds(pl.multiple_of(y * RUN + o, GROUP), n)


def fc2_unit(comm, pos, g, wa):
    r0 = pos.c * HALF
    x, y, z = pos.x, pos.y, pos.z
    full = pl.ds(pl.multiple_of(r0, GROUP), HALF)
    rows = (pl.ds(pl.multiple_of(r0, GROUP), RUN), pl.ds(pl.multiple_of(r0 + RUN, GROUP), RUN))
    two = (pl.ds(0, 2), pl.ds(2, 2))
    ca, cb = pl.ds(0, wa), pl.ds(wa, F2_COLS - wa)

    def cc(i):
        return pl.ds(pl.multiple_of(F2_COLS + i * LANE, LANE), LANE)

    rings_a = [Ring(comm, pos, 'y', lambda i: g.at[z, i, full, ca], lambda i, h: g.at[z, i, rows[h], ca]),
               Ring(comm, pos, 'z', lambda i: g.at[i, :, full, ca], lambda i, h: g.at[i, two[h], full, ca])]
    rings_b = [Ring(comm, pos, 'z', lambda i: g.at[i, y, full, cb], lambda i, h: g.at[i, y, rows[h], cb]),
               Ring(comm, pos, 'y', lambda i: g.at[:, i, full, cb], lambda i, h: g.at[two[h], i, full, cb])]
    rings_c = [Ring(comm, pos, 'y', lambda i: g.at[z, i, full, cc(x)], lambda i, h: g.at[z, i, rows[h], cc(x)]),
               Ring(comm, pos, 'z', lambda i: g.at[i, :, full, cc(x)], lambda i, h: g.at[i, two[h], full, cc(x)]),
               Ring(comm, pos, 'x', lambda i: g.at[:, :, full, cc(i)], lambda i, h: g.at[two[h], :, full, cc(i)])]
    def across(c):
        r = pl.ds(pl.multiple_of(c * HALF, GROUP), HALF)
        return [g.at[:, :, r, k] for k in (ca, cb, pl.ds(F2_COLS, RING * LANE))]

    return (rings_a, rings_b, rings_c), across(pos.c), across(1 - pos.c)


class Unit:
    def __init__(self, comm, pos, parts):
        self.rings, self.mine, self.other = parts
        self.comm = comm
        self.k = comm.take(3)
        self.sib = pos.dev(c=1 - pos.c)

    def across(self, i, refs):
        return self.comm.copy(refs[i], refs[i], self.k + i, self.sib)

    def stage(self, i, n):
        r = self.rings[i]
        if n == 2 * len(r):
            r[-1].end()
            self.across(i, self.mine).start()
        elif n == 2 * len(r) + 1:
            self.across(i, self.other).wait_recv()
        elif n % 2:
            r[n // 2].mid()
        else:
            if n:
                r[n // 2 - 1].end()
            r[n // 2].start()

    def drain(self):
        for i in range(3):
            for r in self.rings[i]:
                r.drain()
            self.across(i, self.mine).wait_send()


def mod_rings(comm, pos, h):
    y, z = pos.y, pos.z
    two, big = (pl.ds(0, 2), pl.ds(2, 2)), (pl.ds(0, HALF), pl.ds(HALF, HALF))
    ca, cb = pl.ds(0, RING * LANE), pl.ds(RING * LANE, 3 * LANE)
    return ([Ring(comm, pos, 'z', lambda i: h.at[i, rows_of(y), ca], lambda i, k: h.at[i, rows_of(y, k), ca]),
             Ring(comm, pos, 'y', lambda i: h.at[:, rows_of(i), ca], lambda i, k: h.at[two[k], rows_of(i), ca])],
            [Ring(comm, pos, 'y', lambda i: h.at[z, rows_of(i), cb], lambda i, k: h.at[z, rows_of(i, k), cb]),
             Ring(comm, pos, 'z', lambda i: h.at[i, :, cb], lambda i, k: h.at[i, big[k], cb])])


def entry_barrier(pos):
    bar = pltpu.get_barrier_semaphore()
    peers = [pos.dev(x=step4(pos.x, k)) for k in (1, 2, 3)]
    peers += [pos.dev(x=step4(pos.x, k), c=1 - pos.c) for k in (0, 1, 2, 3)]
    peers += [pos.dev(y=step4(pos.y, k)) for k in (1, -1)]
    peers += [pos.dev(z=step4(pos.z, k)) for k in (1, -1)]
    for p in peers:
        pl.semaphore_signal(bar, inc=1, device_id=p, device_id_type=MESH)
    pl.semaphore_wait(bar, len(peers))


HIDDEN = 1152
ROWS = 1024
HEAD = 72
HEADS = 16
LN_EPS = 1e-6
LOG2E = 1.4426950408889634


def ln_mod(v, shift, scale):
    mean = jnp.mean(v, axis=-1, keepdims=True)
    cen = v - mean
    var = jnp.mean(cen * cen, axis=-1, keepdims=True)
    return ((cen * lax.rsqrt(var + LN_EPS)) * (1.0 + scale) + shift).astype(jnp.bfloat16)


def piece(m_ref, l, s, j):
    return m_ref[l, pl.ds(s, 1), j * HIDDEN:(j + 1) * HIDDEN]


LT = 128


def norm1(src, m_ref, l, u):
    def body(i, _):
        rows = pl.ds(pl.multiple_of(i * LT, LT), LT)
        s = i // (TILE // LT)
        u[rows, :] = ln_mod(src[rows, :].astype(jnp.float32), piece(m_ref, l, s, 0), piece(m_ref, l, s, 1))
        return 0
    lax.fori_loop(0, ROWS // LT, body, 0)


def qkv_tiles(u, w, b, l, big, tick):
    def tile(cols, width):
        wt = w[:, :, cols].reshape(HIDDEN, width)
        for r in range(0, ROWS, QT):
            acc = jnp.dot(u[r:r + QT, :], wt, preferred_element_type=jnp.float32)
            big[r:r + QT, cols] = (acc + b[l:l + 1, cols].astype(jnp.float32)).astype(jnp.bfloat16)

    def body(n, _):
        tile(pl.ds(pl.multiple_of(n * QT, QT), QT), QT)
        tick(n)
        return 0
    lax.fori_loop(0, 6, body, 0)
    tile(slice(6 * QT, 6 * QT + 384), 384)


def attend(big, o, tick, n=RING):
    lane = lax.broadcasted_iota(jnp.int32, (1, TILE), 1)
    cst = (HEAD ** -0.5) * LOG2E

    def body(s, _):
        rows = pl.ds(pl.multiple_of(s * TILE, TILE), TILE)
        cur, cur_t = None, -1
        for h in range(HEADS):
            st = HEAD * h
            t0 = st // LANE
            off = st - t0 * LANE
            wd = LANE if off + HEAD <= LANE else 2 * LANE
            lo = t0 * LANE
            keep = jnp.logical_and(lane[:, :wd] >= off, lane[:, :wd] < off + HEAD)
            msk = jnp.where(keep, 1.0, 0.0).astype(jnp.bfloat16)
            q = big[rows, lo:lo + wd] * msk
            k = big[rows, HIDDEN + lo:HIDDEN + lo + wd]
            v = big[rows, 2 * HIDDEN + lo:2 * HIDDEN + lo + wd]
            sc = lax.dot_general(q, k, (((1,), (1,)), ((), ())), preferred_element_type=jnp.float32)
            mx = jnp.max(sc, axis=-1, keepdims=True)
            e = jnp.exp2((sc - mx) * cst)
            inv = 1.0 / jnp.sum(e, axis=-1, keepdims=True)
            p = (e * inv).astype(jnp.bfloat16)
            r = jnp.dot(p, v, preferred_element_type=jnp.float32)
            first = r[:, :LANE]
            if cur_t == t0 and off > 0:
                first = jnp.where(lane[:, :LANE] >= off, first, cur)
            if wd == LANE:
                cur, cur_t = first, t0
                if off + HEAD == LANE:
                    o[rows, lo:lo + LANE] = cur.astype(jnp.bfloat16)
                    cur, cur_t = None, -1
            else:
                o[rows, lo:lo + LANE] = first.astype(jnp.bfloat16)
                cur, cur_t = r[:, LANE:], t0 + 1
        tick(s)
        return 0
    lax.fori_loop(0, n, body, 0)


def proj_tiles(o, w, b, m_ref, l, src, x1, u, tick):
    def body(s, _):
        rows = pl.ds(pl.multiple_of(s * TILE, TILE), TILE)
        y = jnp.dot(o[rows, :], w[:, :, 3 * HIDDEN:].reshape(HIDDEN, HIDDEN), preferred_element_type=jnp.float32) + b[l:l + 1, :].astype(jnp.float32)
        v = (src[rows, :].astype(jnp.float32) + piece(m_ref, l, s, 2) * y).astype(jnp.bfloat16)
        x1[rows, :] = v
        u[rows, :] = ln_mod(v.astype(jnp.float32), piece(m_ref, l, s, 3), piece(m_ref, l, s, RING))
        tick(s)
        return 0
    lax.fori_loop(0, RING, body, 0)


def gelu(v):
    return 0.5 * v * (1.0 + jnp.tanh(0.7978845608028654 * (v + 0.044715 * (v * v * v))))


def fc1_tiles(u, w, b, l, big, tick):
    def body(n, _):
        cols = pl.ds(pl.multiple_of(n * QT, QT), QT)
        wt = w[:, :, cols].reshape(HIDDEN, QT)
        for r in range(0, ROWS, QT):
            acc = jnp.dot(u[r:r + QT, :], wt, preferred_element_type=jnp.float32)
            big[r:r + QT, cols] = gelu(acc + b[l:l + 1, cols].astype(jnp.float32)).astype(jnp.bfloat16)
        tick(n)
        return 0
    lax.fori_loop(0, 9, body, 0)


def fc2_tiles(big, w, b, m_ref, l, x1, dst, tick):
    def body(s, _):
        rows = pl.ds(pl.multiple_of(s * TILE, TILE), TILE)
        y = jnp.dot(big[rows, :], w[...].reshape(RING * HIDDEN, HIDDEN), preferred_element_type=jnp.float32) + b[l:l + 1, :].astype(jnp.float32)
        dst[rows, :] = (x1[rows, :].astype(jnp.float32) + piece(m_ref, l, s, 5) * y).astype(jnp.bfloat16)
        tick(s)
        return 0
    lax.fori_loop(0, RING, body, 0)


class Fan:
    def __init__(self, comm, pos, src, dst):
        self.comm, self.pos, self.src, self.dst = comm, pos, src, dst
        self.b = comm.take(GROUP)
        self.p = pos.x * 2 + pos.c

    def peer(self, k):
        q = lax.rem(self.p + k + GROUP, GROUP)
        return q, self.pos.dev(x=q // 2, c=lax.rem(q, 2))

    def put(self, k):
        q, dev = self.peer(k)
        return self.comm.copy(self.src(q), self.dst.at[self.p], self.b + k, dev)

    def start(self):
        for k in ORDER:
            self.put(k).start()

    def wait(self):
        for k in ORDER:
            q, dev = self.peer(-k)
            self.comm.copy(self.src(q), self.dst.at[q], self.b + k, dev).wait_recv()

    def drain(self):
        for k in ORDER:
            self.put(k).wait_send()


ORDER = range(1, GROUP)


class Scatter:
    def __init__(self, comm, pos, pieces, dst):
        self.comm, self.pos, self.pieces, self.dst = comm, pos, pieces, dst
        self.n = len(pieces(0, 0, 0))
        self.b = comm.take(GROUP * self.n)

    def each(self):
        for c in range(2):
            for d in (1, 3, 2, 0):
                x = step4(self.pos.x, d)
                for i, (src, at) in enumerate(self.pieces(x, c, self.pos.c)):
                    yield c, d, i, x, src, at

    def ends(self, d, i, at):
        return self.dst.at[2 * self.pos.x + self.pos.c, :, :, at], self.comm.rsem.at[self.b + (self.pos.c * RING + d) * self.n + i]

    def far(self, c, d, i, x, src, at):
        dst, r = self.ends(d, i, at)
        return pltpu.make_async_remote_copy(src_ref=src, dst_ref=dst, send_sem=self.comm.ssem.at[self.b + (c * RING + d) * self.n + i], recv_sem=r,
                                            device_id=self.pos.dev(x=x, c=c), device_id_type=MESH)

    def near(self, c, d, i, x, src, at):
        return pltpu.make_async_copy(src, *self.ends(d, i, at))

    def start(self):
        for v in self.each():
            if v[1]:
                self.far(*v).start()
            else:
                pl.when(self.pos.c != v[0])(lambda v=v: self.far(*v).start())
                pl.when(self.pos.c == v[0])(lambda v=v: self.near(*v).start())

    def wait(self):
        for c, d, i, x, src, at in self.each():
            dst = self.dst.at[2 * step4(self.pos.x, -d) + c, :, :, at]
            pltpu.make_async_copy(src, dst, self.comm.rsem.at[self.b + (c * RING + d) * self.n + i]).wait()

    def drain(self):
        for v in self.each():
            if v[1]:
                self.far(*v).wait_send()
            else:
                pl.when(self.pos.c != v[0])(lambda v=v: self.far(*v).wait_send())


class Scatter2:
    def __init__(self, comm, pos, w, dst):
        self.comm, self.pos, self.w, self.dst = comm, pos, w, dst
        self.b = comm.take(GROUP)
        self.slot = lax.rem(pos.x, 2) * 2 + pos.c

    def each(self):
        for d in (1, 3, 2, 0):
            x = step4(self.pos.x, d)
            yield d, 0, x, self.w.at[:, :, pl.ds(0, F2_COLS)], pl.ds(0, F2_COLS)
            yield d, 1, x, self.w.at[:, :, pl.ds(pl.multiple_of((5 + x) * LANE, LANE), LANE)], pl.ds(F2_COLS, LANE)

    def ends(self, i, at):
        return self.dst.at[self.slot, :, :, at], self.comm.rsem.at[self.b + self.slot * 2 + i]

    def far(self, d, i, x, src, at):
        dst, r = self.ends(i, at)
        return pltpu.make_async_remote_copy(src_ref=src, dst_ref=dst, send_sem=self.comm.ssem.at[self.b + d * 2 + i], recv_sem=r,
                                            device_id=self.pos.dev(x=x, c=self.pos.x // 2), device_id_type=MESH)

    def near(self, d, i, x, src, at):
        return pltpu.make_async_copy(src, *self.ends(i, at))

    def start(self):
        mine = self.pos.c == self.pos.x // 2
        for v in self.each():
            if v[0]:
                self.far(*v).start()
            else:
                pl.when(jnp.logical_not(mine))(lambda v=v: self.far(*v).start())
                pl.when(mine)(lambda v=v: self.near(*v).start())

    def wait(self):
        for d, i, x, src, at in self.each():
            pltpu.make_async_copy(src, self.dst.at[d, :, :, at], self.comm.rsem.at[self.b + d * 2 + i]).wait()

    def drain(self):
        mine = self.pos.c == self.pos.x // 2
        for v in self.each():
            if v[0]:
                self.far(*v).wait_send()
            else:
                pl.when(jnp.logical_not(mine))(lambda v=v: self.far(*v).wait_send())


def pack_pieces(k, w_qkv, w_proj, w_fc1):
    def pieces(x, c, _):
        out, to = [], 0
        for o, n, step in slices(0, k):
            o += c * (N_A // 2)
            w = w_fc1 if k else w_qkv
            if k == 0 and o >= 3 * HIDDEN:
                w, o = w_proj, o - 3 * HIDDEN
            out.append((w.at[:, :, pl.ds(pl.multiple_of(o + x * step, LANE), n)], pl.ds(to, n)))
            to += n
        return out
    return pieces


def mod_pieces(w_ada):
    def pieces(x, c, _):
        return [(w_ada.at[:, :, pl.ds(pl.multiple_of(jnp.minimum(7 * (2 * x + c), 47) * LANE, LANE), W_MOD)], pl.ds(0, W_MOD))]
    return pieces


def lay_rows(recv, l, wide, packed, n):
    devs, rows = recv.shape[0], recv.shape[1]

    def body(p, _):
        for r in range(rows):
            wide[pl.ds(p * rows + r, 1), :n] = recv[p, r].astype(jnp.float32)[l:l + 1, :]
        return 0
    lax.fori_loop(0, devs, body, 0)
    packed[:, :n] = wide[:, :n].astype(jnp.bfloat16)


def slices(l, k):
    o, out = 0, []
    for a, b, c in SUBS[l, k]:
        out += [(o, (a + b) * LANE, 0), (o + (a + b) * LANE, c * LANE, c * LANE)]
        o += (a + b + RING * c) * LANE
    return out


def place_pack(pos, packed, g, l, k):
    base = pos.c * (N_A // 2)
    pairs, at = [], 0
    for o, n, step in slices(l, k):
        pairs.append((packed.at[:, pl.ds(at, n)], g.at[pos.z, rows_of(pos.y), pl.ds(pl.multiple_of(base + o + pos.x * step, LANE), n)]))
        at += n
    return pairs


class Modulation:
    def __init__(self, comm, pos, l, h, hv, s_all, b_ref, part, got, m, lsem):
        self.rings = mod_rings(comm, pos, h)
        self.l, self.hv, self.s_all, self.b, self.part, self.got, self.m = l, hv, s_all, b_ref, part, got, m
        self.load = pltpu.make_async_copy(h, hv, lsem)
        self.fan = Fan(comm, pos, lambda q: part.at[q], got)

    def ring(self, c, n):
        r = self.rings[c]
        if n % 2:
            r[n // 2].mid()
        else:
            if n:
                r[n // 2 - 1].end()
            if n < RING:
                r[n // 2].start()

    def drain(self):
        for c in self.rings:
            for q in c:
                q.drain()
        self.fan.drain()

    def stage(self, n):
        if n == 0:
            self.load.start()
        elif n == 1:
            self.load.wait()
            rows = self.s_all[...].reshape(64, HIDDEN).astype(jnp.bfloat16)
            w = self.hv[...].reshape(HIDDEN, W_MOD)
            v = jnp.dot(rows, w, preferred_element_type=jnp.float32) + self.b[self.l:self.l + 1, pl.ds(pl.multiple_of(jnp.minimum(7 * self.fan.p, 47) * LANE, LANE), W_MOD)].astype(jnp.float32)
            self.part[...] = v.astype(jnp.bfloat16).astype(jnp.float32).reshape(GROUP, GROUP, W_MOD)
            self.fan.start()
            self.got[self.fan.p] = self.part[self.fan.p]
        else:
            self.fan.wait()
            for q in range(7):
                self.m[self.l, :, W_MOD * q:W_MOD * (q + 1)] = self.got[q]
            self.m[self.l, :, 7 * W_MOD:6 * HIDDEN] = self.got[7][:, 2 * LANE:]


P, W, X, U, M, N, L, S = range(GROUP)
QKV, ATT, PROJ, FC1, FC2 = range(5)
STEPS = ((QKV, 6, 1.5, 0.8), (ATT, RING, 3.2, 0.0), (PROJ, RING, 1.3, 0.0), (FC1, 9, 1.8, 0.0), (FC2, RING, 3.9, 0.0))
LINK, ACROSS, HOP = 46.6e3, 600e3, 3.8
BLOCK = RUN * TILE


class Plan:
    def __init__(self):
        self.t, self.free, self.done, self.pend, self.slack = HOP, {}, set(), [], 0.0
        self.units = [(l, k, v) for l in range(NL) for k in range(3) for v in SUBS[l, k]]
        self.rank = [(3 * l + k, i) for i, (l, k, _) in enumerate(self.units)]
        self.landed, self.loaded, self.left = {}, {}, {}
        self.pre, self.slots = [], []
        for k in range(RING):
            self.add(STARTS[k], (P, k))
        self.add(7.0, (S,))
        self.emit = self.pre
        for l in range(NL):
            self.until((N, l))
            self.t += 2.5
            for st, n, each, tail in STEPS:
                k = {QKV: 0, FC1: 1, FC2: 2}.get(st)
                if k is not None:
                    self.until((L, l, k))
                    self.t = max(self.t, self.loaded[l, k])
                for i in range(n):
                    self.t += each
                    if i == n - 1 and st >= PROJ:
                        self.done.add((L, l, st - PROJ, l))
                    self.emit = []
                    self.slack = 1.0
                    self.catch_up()
                    self.slots.append(((l, st, i), self.emit))
                self.t += tail

    def add(self, when, action):
        k = action[0]
        if k in (U, L):
            rank = self.rank[action[1]]
        elif k == S:
            rank = (0, -2)
        else:
            rank = (3 * action[1], 0) if k in (M, N) else (action[1] % 3, -action[1] // 3)
        self.pend.append((when, rank, action))

    def due(self, p):
        return p[0] + (self.slack if p[2][0] in (U, M, W, X) else 0)

    def allowed(self, a):
        if a[0] == L and self.units[a[1]][0]:
            l, k, _ = self.units[a[1]]
            return (L, l - 1, k, l - 1) in self.done
        if a[0] == N and a[2] == 1:
            return (S,) in self.done
        if a[0] == N and a[2] == 0 and a[1]:
            return (N, a[1] - 1) in self.done
        return True

    def catch_up(self):
        while True:
            c = [p for p in self.pend if self.due(p) <= self.t and self.allowed(p[2])]
            if not c:
                return
            p = min(c, key=lambda v: (v[1], v[0]))
            self.pend.remove(p)
            self.emit.append(p[2])
            self.act(*p[2])

    def until(self, tag):
        self.slack = 0.0
        while True:
            self.catch_up()
            if tag in self.done:
                return
            self.t = max(self.t, min(p[0] for p in self.pend if self.allowed(p[2])))

    def both(self, link, size, rate=LINK):
        self.free[link] = max(self.t, self.free.get(link, self.t)) + size / rate
        return self.free[link] + HOP

    def ring(self, a, chain, size, n):
        if n == 2 * len(chain):
            return True
        half = size * RING ** (n // 2) / 2
        self.add(self.both(chain[n // 2], half), a + (n + 1,))
        if n % 2 == 0:
            self.both(chain[n // 2], half)

    def act(self, kind, *n):
        if kind == P:
            k, = n
            b = (W_F2, W_MOD)[k > 2] if k > 1 else width(0, k)
            self.add(self.both(0, HALF * b), (W, k))
        elif kind == W:
            self.t += 1.5
            self.add(self.t + 1.5, (X,) + n)
        elif kind == X:
            k, = n
            for l in range(NL):
                at = max(self.t, STARTS[RING + k] * l)
                if k == 3:
                    for c in range(2):
                        self.add(at, (M, l, c, 0))
                for u, own in enumerate(self.units):
                    if own[:2] == (l, k):
                        for c in COLOURS:
                            self.add(at, (U, u, c, 0))
        elif kind == U:
            u, c, s = n
            l, k, v = self.units[u]
            size = v[c] * BLOCK * (2 if k == 2 else 1)
            chain = ((1, 2), (2, 1), (1, 2, 0))[c]
            if s == 2 * len(chain) + 1:
                self.landed[u] = self.landed.get(u, 0) + 1
                if self.landed[u] == 3:
                    self.add(self.t, (L, u))
            elif self.ring((U, u, c), chain, size, s):
                self.add(self.both(ACROSS, size * RING ** len(chain), ACROSS), (U, u, c, s + 1))
        elif kind == M:
            l, c, s = n
            if self.ring((M, l, c), ((2, 1), (1, 2))[c], (RING, 3)[c] * BLOCK, s):
                self.left[l] = self.left.get(l, 0) + 1
                if self.left[l] == 2:
                    self.add(self.t, (N, l, 0))
        elif kind == N:
            l, s = n
            if s == 2:
                self.done.add((N, l))
            else:
                self.t += 2.0 * s
                self.add(self.t + (4.5 if s else 2.5), (N, l, s + 1))
        elif kind == L:
            l, k, _ = self.units[n[0]]
            n_k = len(SUBS[l, k])
            self.loaded[l, k] = self.t + 1 + 3.5 / n_k
            self.left[L, l, k] = self.left.get((L, l, k), 0) + 1
            if self.left[L, l, k] == n_k:
                self.done.add((L, l, k))
        else:
            self.done.add((S,))


def step_kernel(x_ref, cond, w_ada, w_qkv, w_proj, w_fc1, w_fc2, ba, bq, bp, b1, b2, out, *refs):
    packs = (refs[0:RING], refs[RING:GROUP])
    u, x1, big, wq, wf, wg, rq, rf, r2, rm, wide, wide2, s_ref, s_all, hv, part, got, m, ssem, rsem, lsem, wsem = refs[GROUP:-GROUP]
    packed = (refs[-GROUP:-RING], refs[-RING:])
    plan = Plan()
    pos = Pos()
    comm = Comm(ssem, rsem)
    bufs = (wq, wf, wg)
    fan_s = Fan(comm, pos, lambda q: s_ref, s_all)
    units, mods, loads, owner = [], [], [], []
    recvs = (rq, rf, r2, rm)
    fans = (Scatter(comm, pos, pack_pieces(0, w_qkv, w_proj, w_fc1), rq), Scatter(comm, pos, pack_pieces(1, w_qkv, w_proj, w_fc1), rf),
            Scatter2(comm, pos, w_fc2, r2), Scatter(comm, pos, mod_pieces(w_ada), rm))
    for l in range(NL):
        gq, gf, g2, gm = packs[l]
        mods.append(Modulation(comm, pos, l, gm, hv, s_all, ba, part.at[l], got.at[l], m, lsem.at[RING * GROUP + l]))
        for k in range(3):
            off, g, buf = 0, packs[l][k], bufs[k]
            for a, b, c in SUBS[l, k]:
                if k == 2:
                    units.append(Unit(comm, pos, fc2_unit(comm, pos, g, a * LANE)))
                    pairs = [(g, buf)]
                else:
                    units.append(Unit(comm, pos, pack_unit(comm, pos, g, off, a * LANE, b * LANE, c * LANE)))
                    n = (a + b + RING * c) * LANE
                    cols = [pl.ds(h * (N_A // 2) + off, n) for h in range(2)]
                    pairs = [(g.at[:, :, q], buf.at[:, :, q]) for q in cols]
                    off += n
                first = len(sum(loads, []))
                loads.append([pltpu.make_async_copy(s, d, wsem.at[first + i]) for i, (s, d) in enumerate(pairs)])
                owner.append((l, k))

    def ready(l, k):
        for own, cps in zip(owner, loads):
            if own == (l, k):
                for cp in cps:
                    cp.wait()

    def placing(i):
        pairs = []
        for l in range(NL):
            g, block = packs[l][i], packed[l][i]
            if i == 3:
                pairs.append((block, g.at[pos.z, rows_of(pos.y)]))
            elif i < 2:
                pairs += place_pack(pos, block, g, l, i)
            else:
                full = pl.ds(pl.multiple_of(pos.c * HALF, GROUP), HALF)
                pairs += [(block.at[:, pl.ds(0, F2_COLS)], g.at[pos.z, pos.y, full, pl.ds(0, F2_COLS)]),
                          (block.at[:, pl.ds(F2_COLS, LANE)], g.at[pos.z, pos.y, full, pl.ds(pl.multiple_of(F2_COLS + pos.x * LANE, LANE), LANE)])]
        return [pltpu.make_async_copy(a, b, lsem.at[i * GROUP + k]) for k, (a, b) in enumerate(pairs)]

    def act(kind, *n):
        if kind == P:
            fans[n[0]].start()
        elif kind == W:
            i, = n
            fans[i].wait()
            for l in range(NL):
                lay_rows(recvs[i], l, wide2 if i == 2 else wide, packed[l][i], recvs[i].shape[-1])
            for cp in placing(i):
                cp.start()
        elif kind == X:
            for cp in placing(*n):
                cp.wait()
        elif kind == U:
            units[n[0]].stage(n[1], n[2])
        elif kind == M:
            mods[n[0]].ring(n[1], n[2])
        elif kind == N:
            mods[n[0]].stage(n[1])
        elif kind == L:
            for cp in loads[n[0]]:
                cp.start()
        else:
            fan_s.wait()

    def ticker(l, stage):
        def tick(i):
            for (sl, ss, k), actions in plan.slots:
                if sl == l and ss == stage and actions:
                    @pl.when(i == k)
                    def _():
                        for v in actions:
                            act(*v)
        return tick

    s_ref[...] = jnp.zeros_like(s_ref)
    cv = cond[...].astype(jnp.float32)
    s_ref[0:RING, :] = jax.nn.silu(cv).astype(jnp.bfloat16).astype(jnp.float32)
    entry_barrier(pos)
    fan_s.start()
    s_all[fan_s.p] = s_ref[...]
    for v in plan.pre:
        act(*v)
    src = x_ref
    for l in range(NL):
        norm1(src, m, l, u)
        ready(l, 0)
        qkv_tiles(u, wq, bq, l, big, ticker(l, QKV))
        attend(big, u, ticker(l, ATT))
        proj_tiles(u, wq, bp, m, l, src, x1, u, ticker(l, PROJ))
        ready(l, 1)
        fc1_tiles(u, wf, b1, l, big, ticker(l, FC1))
        ready(l, 2)
        fc2_tiles(big, wg, b2, m, l, x1, out, ticker(l, FC2))
        src = out
    fan_s.drain()
    for v in fans:
        v.drain()
    for v in mods:
        v.drain()
    for v in units:
        v.drain()


N_SEM = GROUP * (3 + RING * NL) + 16 * sum(len(SUBS[0, k]) for k in range(2)) + 45 * sum(len(v) for v in SUBS.values()) + 8 * GROUP


def run_step(x, cond, w_ada, w_qkv, w_proj, w_fc1, w_fc2, ba, bq, bp, b1, b2):
    bf, f32 = jnp.bfloat16, jnp.float32
    shapes = [(RING, PLANE, N_A), (RING, PLANE, N_A), (RING, RING, PLANE, HIDDEN), (RING, PLANE, W_MOD)] * NL
    hbm = pl.BlockSpec(memory_space=pl.ANY)
    vm = pl.BlockSpec(memory_space=pltpu.VMEM)
    dma = pltpu.SemaphoreType.DMA
    wide = [width(0, k) for k in range(2)]
    return pl.pallas_call(
        step_kernel,
        out_shape=[jax.ShapeDtypeStruct((ROWS, HIDDEN), bf)] + [jax.ShapeDtypeStruct(s, bf) for s in shapes],
        in_specs=[vm, vm] + [hbm] * 5 + [vm] * 5, out_specs=[vm] + [hbm] * GROUP,
        scratch_shapes=[pltpu.VMEM((ROWS, HIDDEN), bf), pltpu.VMEM((ROWS, HIDDEN), bf), pltpu.VMEM((ROWS, N_A), bf),
                        pltpu.VMEM((RING, PLANE, N_A), bf), pltpu.VMEM((RING, PLANE, N_A), bf), pltpu.VMEM((RING, RING, PLANE, HIDDEN), bf),
                        pltpu.VMEM((GROUP, 9, NL, wide[0]), bf), pltpu.VMEM((GROUP, 9, NL, wide[1]), bf), pltpu.VMEM((RING, 36, NL, W_F2), bf), pltpu.VMEM((GROUP, 9, NL, W_MOD), bf),
                        pltpu.VMEM((RUN, max(wide)), f32), pltpu.VMEM((HALF, W_F2), f32),
                        pltpu.VMEM((GROUP, HIDDEN), f32), pltpu.VMEM((GROUP, GROUP, HIDDEN), f32), pltpu.VMEM((RING, PLANE, W_MOD), bf),
                        pltpu.VMEM((NL, GROUP, GROUP, W_MOD), f32), pltpu.VMEM((NL, GROUP, GROUP, W_MOD), f32), pltpu.VMEM((NL, GROUP, 6 * HIDDEN), f32),
                        dma((N_SEM,)), dma((N_SEM,)), dma((5 * GROUP,)), dma((2 * sum(len(v) for v in SUBS.values()),))]
        + [pltpu.VMEM((n, c), bf) for _ in range(NL) for n, c in ((RUN, wide[0]), (RUN, wide[1]), (HALF, W_F2), (RUN, W_MOD))],
        compiler_params=pltpu.CompilerParams(collective_id=0, has_side_effects=True, vmem_limit_bytes=67043328),
        name='dit_blocks',
    )(x, cond, w_ada, w_qkv, w_proj, w_fc1, w_fc2, ba, bq, bp, b1, b2)[0]


def solution(mesh):
    batch_spec = PartitionSpec(('dp', 'fsdp'), None, None)
    cond_spec = PartitionSpec(('dp', 'fsdp'), None)
    shard_spec = PartitionSpec(None, 'fsdp', None)
    bias_spec = PartitionSpec(None, None)

    def local_run(latents, cond_emb, w_ada, b_ada, w_qkv, b_qkv, w_proj, b_proj, w_fc1, b_fc1, w_fc2, b_fc2):
        y = run_step(latents.reshape(ROWS, HIDDEN), cond_emb, *[jnp.swapaxes(w, 0, 1) for w in (w_ada, w_qkv, w_proj, w_fc1, w_fc2)], b_ada, b_qkv, b_proj, b_fc1, b_fc2)
        return y.reshape(latents.shape)

    in_specs = (batch_spec, cond_spec, shard_spec, bias_spec, shard_spec, bias_spec, shard_spec, bias_spec, shard_spec, bias_spec, shard_spec, bias_spec)
    return jax.shard_map(local_run, mesh=mesh, in_specs=in_specs, out_specs=batch_spec, check_vma=False)
```
